32 devices in a mesh: turn: 4 (over y, core), blk: 4 (over z), strip: 2 (over x).
Axes of the slice: x: 2, y: 2, z: 4, core: 2. Of those that a mesh axis runs over, the one named last changes fastest.
Arguments:
- echoes: bfloat16 [2, 256, 32768], P(None, 'blk', ('turn', 'strip')), may hold values from -6 to 6
- filters: bfloat16 [2, 8, 32768], P(None, 'blk'), may hold values from -6 to 6
- slab_index: int32 [256], P(('blk', 'turn')), may hold values from 0 to 7
- shifts: int32 [256], P(('blk', 'turn')), may hold values from 0 to 32767
Outputs:
- focused: float32 [2, 256, 32768], P(None, ('blk', 'turn'), 'strip')
The draws below stay inside these ranges and needn't reach their ends.
All inputs are finite; a program needn't handle non-finite values.
Results may differ from the reference program's by a relative error of at most 0.0003.
Values may be sent and summed in bfloat16 or wider, within the bound.
No kernel may reach another device: no remote copies, remote signals or barrier semaphores. Data moves between devices by JAX's collectives and lax.ppermute only.
A program may use at most 128 MiB of HBM per device.

```python
import jax
import jax.numpy as jnp
from jax import lax

NA = 32768
NR = 256
NS = 8


def plant(entries, stream_key, smallest, largest):
    dims = entries.shape
    place = [jax.random.randint(jax.random.fold_in(stream_key, axis), (), 0, dims[axis]) for axis in range(len(dims))]
    entries = entries.at[tuple(place)].set(smallest)
    longest = dims.index(max(dims))
    place[longest] = (place[longest] + 1) % dims[longest]
    return entries.at[tuple(place)].set(largest)


def block_scale(own_key, extent, split, smallest, high):
    loudness, own = 1.0, jax.random.fold_in(own_key, 6)
    for dim, blocks in split:
        steps = jnp.exp(jax.random.uniform(jax.random.fold_in(own, dim), (blocks,), jnp.float32, smallest / len(split), high / len(split)))
        loudness = loudness * jnp.repeat(steps, extent[dim] // blocks).reshape([-1 if axis == dim else 1 for axis in range(len(extent))])
    return loudness


def scatter_about(rng, shape, scale, limit, split=(), kind=jnp.bfloat16):
    values = jax.random.normal(rng, shape, jnp.float32) * scale
    if len(split) > 0:
        values = block_scale(rng, shape, split, -0.22, 0.18) * values
    return jnp.clip(values, min=-limit, max=limit).astype(kind)


def setup_inputs(seed: int = 0) -> dict:
    key_of = jax.random.split(jax.random.key(seed), 5)
    echoes = scatter_about(key_of[0], (2, NR, NA), 1.0, 6.0, ((1, 4), (2, 8)))
    filters = scatter_about(key_of[1], (2, NS, NA), 1.0, 6.0, ((1, 4),))
    slab_index = plant(jax.random.randint(key_of[2], (NR,), 0, NS), jax.random.fold_in(key_of[2], 1), 0, NS - 1).astype(jnp.int32)
    shifts = plant(jax.random.randint(key_of[3], (NR,), 0, NA), jax.random.fold_in(key_of[3], 1), 0, NA - 1).astype(jnp.int32)
    return dict(echoes=echoes, filters=filters, slab_index=slab_index, shifts=shifts)


def reference(echoes, filters, slab_index, shifts):
    signal = lax.complex(echoes[0].astype(jnp.float32), echoes[1].astype(jnp.float32))
    spectrum = jnp.fft.fft(signal, axis=1)
    chosen = lax.complex(filters[0][slab_index].astype(jnp.float32), filters[1][slab_index].astype(jnp.float32))
    image = jnp.fft.ifft(spectrum * chosen, axis=1)
    positions = (jnp.arange(NA, dtype=jnp.int32)[None, :] - shifts[:, None].astype(jnp.int32)) % NA
    rolled = jnp.take_along_axis(image, positions, axis=1)
    return jnp.stack([jnp.real(rolled), jnp.imag(rolled)]).astype(jnp.float32)
```

```python
import functools
import math

import jax
import jax.numpy as jnp
import numpy as np
from jax import lax
from jax.experimental import pallas as pl
from jax.experimental.pallas import tpu as pltpu
from jax.sharding import PartitionSpec as P

LANES = 128
CHUNKS = (8, 8)


def hi_lo(table):
    high = table.astype(jnp.bfloat16)
    low = (table - high.astype(np.float64)).astype(jnp.bfloat16)
    return high, low


def block_matrix(phase, sign):
    cos, sin = np.cos(phase), sign * np.sin(phase)
    return np.concatenate([np.concatenate([cos, -sin], 1), np.concatenate([sin, cos], 1)], 0)


@functools.lru_cache(maxsize=None)
def tables(length, sources, out_len):
    slow = length // LANES
    part = slow // sources
    out_slow = out_len // LANES
    q = np.arange(slow)
    lane = np.arange(LANES)
    first = block_matrix(2 * np.pi * (q[:, None] * q[None, :] % slow) / slow, -1.0)
    first = first.reshape(2 * slow, 2, sources, part).transpose(0, 2, 1, 3).reshape(2 * slow, 2 * slow)
    lane_phase = 2 * np.pi * (lane[:, None] * lane[None, :] % LANES) / LANES
    middle = block_matrix(lane_phase, -1.0).T
    back = block_matrix(lane_phase, 1.0).T
    last = block_matrix(2 * np.pi * (q[:out_slow, None] * q[None, :] % slow) / slow, 1.0) / length
    twist = 2 * np.pi * (q[:, None] * lane[None, :]) / length
    first_hi, first_lo = hi_lo(first)
    mid_hi, mid_lo = hi_lo(middle)
    back_hi, back_lo = hi_lo(back)
    last_hi, last_lo = hi_lo(last)
    return dict(
        first=np.concatenate([first_hi, first_lo], 1),
        middle=np.concatenate([mid_hi, mid_hi, mid_lo], 0),
        back=np.concatenate([back_hi, back_hi, back_lo], 0),
        last=np.concatenate([last_hi, last_lo], 1),
        twist=np.stack([np.cos(twist), np.sin(twist)]).astype(np.float32),
    )


def split(value):
    high = value.astype(jnp.bfloat16)
    return high, (value - high.astype(jnp.float32)).astype(jnp.bfloat16)


def dot(a, b):
    return jnp.dot(a, b, preferred_element_type=jnp.float32)


def focus_kernel(sources, rows, row0, slow, out_slow, *refs):
    scalars = refs[0]
    blocks = refs[1 : 1 + sources]
    (filt, ramp_c, ramp_d, first, middle, back, last, twist, held, out, x, y, w, sem) = refs[1 + sources :]
    me, core = scalars[0], scalars[1]
    copies = []
    for d in range(sources):
        copy = pltpu.make_async_copy(blocks[d], x.at[me ^ d], sem.at[d])
        copy.start()
        copies.append(copy)
    for copy in copies:
        copy.wait()
    half = slow // 2
    for pair in range(rows // 2):
        both = (2 * pair, 2 * pair + 1)
        data = jnp.concatenate(
            [
                jnp.concatenate([x[j, p, r] for j in range(sources) for p in range(2)], 0)
                for r in both
            ],
            1,
        )
        stage = dot(first[:, : 2 * slow], data) + dot(first[:, 2 * slow :], data)
        tw_re, tw_im = twist[0], twist[1]
        for i, r in enumerate(both):
            re = stage[:slow, i * LANES : (i + 1) * LANES]
            im = stage[slow:, i * LANES : (i + 1) * LANES]
            new_re, new_im = re * tw_re + im * tw_im, im * tw_re - re * tw_im
            (rh, rl), (ih, il) = split(new_re), split(new_im)
            y[pair, i, :, :] = jnp.concatenate([rh, ih, rl, il], 1)
        mix = y[pair].reshape(2 * slow, 4 * LANES)
        stage = dot(mix, middle[: 4 * LANES]) + dot(mix[:, : 2 * LANES], middle[4 * LANES :])
        for i, r in enumerate(both):
            re = stage[i * slow : (i + 1) * slow, :LANES]
            im = stage[i * slow : (i + 1) * slow, LANES:]
            slab = scalars[2 + row0 + r]
            h_re = jnp.concatenate([filt[p ^ core, slab, 0] for p in range(2)], 0).astype(jnp.float32)
            h_im = jnp.concatenate([filt[p ^ core, slab, 1] for p in range(2)], 0).astype(jnp.float32)
            re, im = re * h_re - im * h_im, re * h_im + im * h_re
            v_re, v_im = ramp_d[0, row0 + r][None, :], ramp_d[1, row0 + r][None, :]
            re, im = re * v_re - im * v_im, re * v_im + im * v_re
            (rh, rl), (ih, il) = split(re), split(im)
            y[pair, i, :, :] = jnp.concatenate([rh, ih, rl, il], 1)
        mix = y[pair].reshape(2 * slow, 4 * LANES)
        stage = dot(mix, back[: 4 * LANES]) + dot(mix[:, : 2 * LANES], back[4 * LANES :])
        for i, r in enumerate(both):
            re = stage[i * slow : (i + 1) * slow, :LANES]
            im = stage[i * slow : (i + 1) * slow, LANES:]
            re, im = re * tw_re - im * tw_im, re * tw_im + im * tw_re
            u_re, u_im = ramp_c[0, :, row0 + r][:, None], ramp_c[1, :, row0 + r][:, None]
            re, im = re * u_re - im * u_im, re * u_im + im * u_re
            (rh, rl), (ih, il) = split(re), split(im)
            w[pair, : 2 * slow, i * LANES : (i + 1) * LANES] = jnp.concatenate([rh, ih], 0)
            w[pair, 2 * slow :, i * LANES : (i + 1) * LANES] = jnp.concatenate([rl, il], 0)
        high = w[pair, : 2 * slow]
        stage = dot(last[:, : 2 * slow], high) + dot(last[:, 2 * slow :], high) + dot(last[:, : 2 * slow], w[pair, 2 * slow :])
        for i, r in enumerate(both):
            for p in range(2):
                for q in range(0, out_slow, 8):
                    out[p, 0, pl.ds(q * 8 + r, 8, stride=8), :] = stage[
                        p * out_slow + q : p * out_slow + q + 8, i * LANES : (i + 1) * LANES
                    ]


def focus(blocks, filt, ramp_c, ramp_d, scalars, held, t, rows, row0, total, slow, out_slow):
    sources = len(blocks)
    part = slow // sources
    vm = pl.BlockSpec(memory_space=pltpu.VMEM)
    hbm = pl.BlockSpec(memory_space=pltpu.HBM)
    sm = pl.BlockSpec(memory_space=pltpu.SMEM)
    tile = row0 // 8
    whole = pl.BlockSpec((2, 1, out_slow * 8, LANES), lambda i: (0, tile, 0, 0))

    def full(a):
        return pl.BlockSpec(a.shape, lambda i: (0,) * a.ndim)

    operands = [filt, ramp_c, ramp_d] + [jnp.asarray(t[k]) for k in ("first", "middle", "back", "last", "twist")]
    aliases = {}
    if held is None:
        held = jnp.zeros((8, LANES), jnp.float32)
    else:
        aliases = {1 + sources + len(operands): 0}
    return pl.pallas_call(
        functools.partial(focus_kernel, sources, rows, row0, slow, out_slow),
        grid=(1,),
        in_specs=[sm] + [hbm] * sources + [full(a) for a in operands] + [hbm],
        out_specs=whole,
        out_shape=jax.ShapeDtypeStruct((2, total // 8, out_slow * 8, LANES), jnp.float32),
        scratch_shapes=[
            pltpu.VMEM((sources, 2, rows, part, LANES), jnp.bfloat16),
            pltpu.VMEM((rows // 2, 2, slow, 4 * LANES), jnp.bfloat16),
            pltpu.VMEM((rows // 2, 4 * slow, 2 * LANES), jnp.bfloat16),
            pltpu.SemaphoreType.DMA((sources,)),
        ],
        input_output_aliases=aliases,
        compiler_params=pltpu.CompilerParams(vmem_limit_bytes=40 * 1024 * 1024),
        cost_estimate=pl.CostEstimate(flops=3 * 10**9, bytes_accessed=8 * 10**6, transcendentals=0),
    )(scalars, *blocks, *operands, held)


def per_device(echoes, filters, slab_index, shifts):
    turns, strips, zones = lax.axis_size("turn"), lax.axis_size("strip"), lax.axis_size("blk")
    turn, strip, zone = lax.axis_index("turn"), lax.axis_index("strip"), lax.axis_index("blk")
    sources = turns * strips
    span = echoes.shape[2]
    length = span * sources
    slow = length // LANES
    part = span // LANES
    total = slab_index.shape[0]
    out_slow = slow // strips
    per_zone = filters.shape[1]
    t = tables(length, sources, length // strips)
    core = turn % 2

    shaped = echoes.reshape(2, turns, total, part, LANES)
    blocks = []
    row0 = 0
    for rows in CHUNKS:
        mine = [None] * sources
        for d in range(sources):
            dt, ds = d // strips, d % strips
            block = lax.dynamic_index_in_dim(shaped, turn ^ dt, axis=1, keepdims=False)[:, row0 : row0 + rows]
            if d:
                pairs = [
                    (a * strips + b, (a ^ dt) * strips + (b ^ ds)) for a in range(turns) for b in range(strips)
                ]
                block = lax.ppermute(block, ("turn", "strip"), pairs)
            mine[d] = block
        blocks.append(mine)
        row0 += rows

    turned = filters.reshape(2, per_zone, LANES, slow).transpose(1, 0, 3, 2)
    half = lax.dynamic_slice_in_dim(turned, core * (slow // 2), slow // 2, axis=2)
    pieces = [half]
    for d in range(1, zones):
        pieces.append(lax.ppermute(half, "blk", [(a, a ^ d) for a in range(zones)]))
    own = jnp.concatenate(pieces, 0)
    other = lax.ppermute(own, "turn", [(a, a ^ 1) for a in range(turns)])
    filt = jnp.stack([own, other])
    local_slab = (slab_index // per_zone ^ zone) * per_zone + slab_index % per_zone

    c = jnp.arange(slow, dtype=jnp.int32)[:, None]
    offset = (shifts + (strips - strip) * (length // strips)) % length
    c_turn = c * offset[None, :] % length
    c_angle = c_turn.astype(jnp.float32) * (2.0 * math.pi / length)
    ramp_c = jnp.stack([jnp.cos(c_angle), -jnp.sin(c_angle)])
    d = jnp.arange(LANES, dtype=jnp.int32)[None, :]
    d_angle = (d * (shifts[:, None] % LANES) % LANES).astype(jnp.float32) * (2.0 * math.pi / LANES)
    ramp_d = jnp.stack([jnp.cos(d_angle), -jnp.sin(d_angle)])
    scalars = jnp.concatenate([jnp.stack([turn * strips + strip, core]).astype(jnp.int32), local_slab])

    held = None
    row0 = 0
    for rows, mine in zip(CHUNKS, blocks):
        held = focus(mine, filt, ramp_c, ramp_d, scalars, held, t, rows, row0, total, slow, out_slow)
        row0 += rows
    tiles = total // 8
    image = held.reshape(2, tiles, out_slow, 8, LANES).transpose(0, 1, 3, 2, 4)
    return image.reshape(2, total, out_slow * LANES)


def solution(mesh):
    in_specs = (
        P(None, "blk", ("turn", "strip")),
        P(None, "blk", None),
        P(("blk", "turn")),
        P(("blk", "turn")),
    )
    out_specs = P(None, ("blk", "turn"), "strip")
    return jax.shard_map(per_device, mesh=mesh, in_specs=in_specs, out_specs=out_specs, check_vma=False)
```

```python
import functools
import math

import jax
import jax.numpy as jnp
import numpy as np
from jax import lax
from jax.experimental import pallas as pl
from jax.experimental.pallas import tpu as pltpu
from jax.sharding import PartitionSpec as P


LANES = 128
CHUNKS = (8, 8)


def hi_lo(table):
    high = table.astype(jnp.bfloat16)
    low = (table - high.astype(np.float64)).astype(jnp.bfloat16)
    return high, low


def block_matrix(phase, sign):
    cos, sin = np.cos(phase), sign * np.sin(phase)
    return np.concatenate([np.concatenate([cos, -sin], 1), np.concatenate([sin, cos], 1)], 0)


@functools.lru_cache(maxsize=None)
def tables(length, sources, out_len):
    slow = length // LANES
    half = slow // 2
    part = half // sources
    out_half = out_len // LANES // 2
    q = np.arange(slow)
    c = np.arange(half)
    lane = np.arange(LANES)
    lane_phase = 2 * np.pi * (lane[:, None] * lane[None, :] % LANES) / LANES
    twist = 2 * np.pi * (q[:, None] * lane[None, :]) / length
    first, last = [], []
    for parity in range(2):
        index = 2 * c + parity
        table = block_matrix(2 * np.pi * (c[:, None] * index[None, :] % slow) / slow, -1.0)
        table = table.reshape(slow, 2, sources, part).transpose(0, 2, 1, 3).reshape(slow, slow)
        first.append(np.stack(hi_lo(table)))
        table = block_matrix(2 * np.pi * (index[:out_half, None] * c[None, :] % slow) / slow, 1.0) / length
        last.append(np.stack(hi_lo(table)))
    middle = np.stack(hi_lo(block_matrix(lane_phase, -1.0).T))
    back = np.stack(hi_lo(block_matrix(lane_phase, 1.0).T))
    parts = [np.stack(first), middle, back, np.stack(last)]
    dots = np.concatenate([a.reshape(-1, a.shape[-1]) for a in parts], 0)
    return dots, np.stack([np.cos(twist), np.sin(twist)]).astype(np.float32)


def split(value):
    high = value.astype(jnp.bfloat16)
    return high, (value - high.astype(jnp.float32)).astype(jnp.bfloat16)


def dot(a, b):
    return jnp.dot(a, b, preferred_element_type=jnp.float32)


def pack_kernel(jobs, total, part, ids, echoes, *refs):
    turn, outs, spread = ids[0], refs[:-1], refs[-1]
    for k, (flip, row0, rows) in enumerate(jobs):
        for row in range(0, rows, 8):
            start = pl.multiple_of((turn ^ flip) * total + row0 + row, 8)
            for p in range(2):
                block = echoes[p, pl.ds(start, 8), :].astype(jnp.float32)
                for q in range(part):
                    spread[k, row // 8, p, q * 8 : (q + 1) * 8] = block[:, q * LANES : (q + 1) * LANES]
    for k, (flip, row0, rows) in enumerate(jobs):
        for row in range(rows):
            for p in range(2):
                for e in range(2):
                    start = e * 8 + row % 8
                    picked = spread[k, row // 8, p, pl.ds(start, part // 2, stride=16), :]
                    outs[k][p, row, e] = picked.astype(jnp.bfloat16)


def pack(ids, echoes, jobs, total, cost):
    part = echoes.shape[2] // LANES
    vm = pl.BlockSpec(memory_space=pltpu.VMEM)
    sm = pl.BlockSpec(memory_space=pltpu.SMEM)
    tiles = max(rows for _, _, rows in jobs) // 8
    return pl.pallas_call(
        functools.partial(pack_kernel, tuple(jobs), total, part),
        in_specs=[sm, vm],
        out_specs=[vm] * len(jobs),
        out_shape=[jax.ShapeDtypeStruct((2, rows, 2, part // 2, LANES), jnp.bfloat16) for _, _, rows in jobs],
        scratch_shapes=[pltpu.VMEM((len(jobs), tiles, 2, part * 8, LANES), jnp.float32)],
        compiler_params=pltpu.CompilerParams(vmem_limit_bytes=12 * 1024 * 1024),
        cost_estimate=pl.CostEstimate(flops=10**6, bytes_accessed=cost, transcendentals=0),
    )(ids, echoes)


def order_kernel(width, ids, dots, twist, out):
    size = dots.shape[1]
    row_ids = lax.broadcasted_iota(jnp.int32, (size, size), 0)
    col_ids = lax.broadcasted_iota(jnp.int32, (size, size), 1)
    order = jnp.where(row_ids == (col_ids ^ (ids[2] * width)), 1.0, 0.0).astype(jnp.bfloat16)
    out[...] = dot(dots[: 4 * size], order).astype(jnp.bfloat16)


def order_tables(ids, dots, twist, width):
    vm = pl.BlockSpec(memory_space=pltpu.VMEM)
    sm = pl.BlockSpec(memory_space=pltpu.SMEM)
    size = dots.shape[1]
    return pl.pallas_call(
        functools.partial(order_kernel, width),
        in_specs=[sm, vm, vm],
        out_specs=vm,
        out_shape=jax.ShapeDtypeStruct((4 * size, size), jnp.bfloat16),
        compiler_params=pltpu.CompilerParams(vmem_limit_bytes=8 * 1024 * 1024),
        cost_estimate=pl.CostEstimate(flops=10**6, bytes_accessed=4 * 10**6, transcendentals=0),
    )(ids, dots, twist)


def turn_kernel(ids, filters, out, turned):
    core = ids[1]
    slabs = filters.shape[1]
    for p in range(2):
        for d in range(LANES):
            at = pl.multiple_of((2 * d + core) * LANES, LANES)
            lanes = filters[p, :, pl.ds(at, LANES)].astype(jnp.float32)
            for slab in range(slabs):
                turned[slab, p, d : d + 1, :] = lanes[slab : slab + 1]
    for p in range(2):
        for slab in range(slabs):
            out[slab, p] = turned[slab, p].T.astype(jnp.bfloat16)


def turn_filters(ids, filters):
    vm = pl.BlockSpec(memory_space=pltpu.VMEM)
    sm = pl.BlockSpec(memory_space=pltpu.SMEM)
    shape = (filters.shape[1], 2, LANES, LANES)
    return pl.pallas_call(
        turn_kernel,
        in_specs=[sm, vm],
        out_specs=vm,
        out_shape=jax.ShapeDtypeStruct(shape, jnp.bfloat16),
        scratch_shapes=[pltpu.VMEM(shape, jnp.float32)],
        compiler_params=pltpu.CompilerParams(vmem_limit_bytes=4 * 1024 * 1024),
        cost_estimate=pl.CostEstimate(flops=10**6, bytes_accessed=2 * 10**6, transcendentals=0),
    )(ids, filters)


def focus_kernel(bases, pieces, rows, row0, slow, out_slow, *refs):
    sources = len(bases)
    scalars = refs[0]
    blocks = refs[1 : 1 + sources]
    own = refs[1 + sources : 1 + sources + pieces]
    other = refs[1 + sources + pieces : 1 + sources + 2 * pieces]
    (
        slow_cos, slow_sin, fast_cos, fast_sin, first_dots_ref, dots, twist, _, out,
        s1, y1, s2, y2, s3, y3, s4, slow_ramp, filt,
    ) = refs[1 + sources + 2 * pieces :]
    core = scalars[0]
    per_zone = own[0].shape[0]
    for k in range(pieces):
        filt[core, k * per_zone : (k + 1) * per_zone] = own[k][...]
        filt[1 - core, k * per_zone : (k + 1) * per_zone] = other[k][...]
    slow_ramp[0] = slow_cos[...].T
    slow_ramp[1] = slow_sin[...].T
    half = slow // 2
    wide = 2 * LANES
    first = [[first_dots_ref.at[pl.ds((2 * e + k) * slow, slow)] for k in range(2)] for e in range(2)]
    base = 4 * slow
    middle = [dots.at[pl.ds(base + k * wide, wide)] for k in range(2)]
    back = [dots.at[pl.ds(base + (2 + k) * wide, wide)] for k in range(2)]
    base += 4 * wide
    last = [[dots.at[pl.ds(base + (2 * e + k) * out_slow, out_slow)] for k in range(2)] for e in range(2)]

    def first_dots(pair):
        for e in range(2):
            data = jnp.concatenate(
                [
                    jnp.concatenate([block[p, base + r, e] for block, base in zip(blocks, bases) for p in range(2)], 0)
                    for r in (2 * pair, 2 * pair + 1)
                ],
                1,
            )
            s1[pair, e] = dot(first[e][0][...], data) + dot(first[e][1][...], data)

    def first_twist(pair):
        for i in range(2):
            lanes = slice(i * LANES, (i + 1) * LANES)
            for part in range(2):
                rows_c = slice(part * half, (part + 1) * half)
                even_re, even_im = s1[pair, 0, :half, lanes], s1[pair, 0, half:, lanes]
                odd_re, odd_im = s1[pair, 1, :half, lanes], s1[pair, 1, half:, lanes]
                if part == 0:
                    re, im = even_re + odd_re, even_im + odd_im
                else:
                    re, im = even_re - odd_re, even_im - odd_im
                tw_re, tw_im = twist[0, rows_c], twist[1, rows_c]
                (rh, rl), (ih, il) = split(re * tw_re + im * tw_im), split(im * tw_re - re * tw_im)
                y1[pair, i, rows_c] = jnp.concatenate([rh, ih, rl, il], 1)

    def lane_dots(pair, source, table, target):
        mix = source[pair].reshape(2 * slow, 2 * wide)
        target[pair] = (
            dot(mix[:, :wide], table[0][...]) + dot(mix[:, wide:], table[0][...]) + dot(mix[:, :wide], table[1][...])
        )

    def respond(pair):
        for i in range(2):
            r = row0 + 2 * pair + i
            slab = scalars[1 + r]
            v_re, v_im = fast_cos[r : r + 1], fast_sin[r : r + 1]
            for part in range(2):
                rows_s = slice(i * slow + part * half, i * slow + (part + 1) * half)
                re, im = s2[pair, rows_s, :LANES], s2[pair, rows_s, LANES:]
                h_re = filt[part, slab, 0].astype(jnp.float32)
                h_im = filt[part, slab, 1].astype(jnp.float32)
                re, im = re * h_re - im * h_im, re * h_im + im * h_re
                (rh, rl), (ih, il) = split(re * v_re - im * v_im), split(re * v_im + im * v_re)
                y2[pair, i, part * half : (part + 1) * half] = jnp.concatenate([rh, ih, rl, il], 1)

    def back_twist(pair):
        for i in range(2):
            r = row0 + 2 * pair + i
            lanes = slice(i * LANES, (i + 1) * LANES)
            parts = []
            for part in range(2):
                rows_c = slice(part * half, (part + 1) * half)
                rows_s = slice(i * slow + part * half, i * slow + (part + 1) * half)
                re, im = s3[pair, rows_s, :LANES], s3[pair, rows_s, LANES:]
                tw_re, tw_im = twist[0, rows_c], twist[1, rows_c]
                re, im = re * tw_re - im * tw_im, re * tw_im + im * tw_re
                u_re, u_im = slow_ramp[0, rows_c, r : r + 1], slow_ramp[1, rows_c, r : r + 1]
                parts.append((re * u_re - im * u_im, re * u_im + im * u_re))
            (a_re, a_im), (b_re, b_im) = parts
            for e, (re, im) in enumerate(((a_re + b_re, a_im + b_im), (a_re - b_re, a_im - b_im))):
                (rh, rl), (ih, il) = split(re), split(im)
                y3[pair, e, 0, :, lanes] = jnp.concatenate([rh, ih], 0)
                y3[pair, e, 1, :, lanes] = jnp.concatenate([rl, il], 0)

    def last_dots(pair):
        for e in range(2):
            high, low = y3[pair, e, 0], y3[pair, e, 1]
            s4[pair, e] = (
                dot(last[e][0][...], high) + dot(last[e][1][...], high) + dot(last[e][0][...], low)
            )

    def store(pair):
        count = out_slow // 2
        for i in range(2):
            r = (row0 + 2 * pair + i) % 8
            for e in range(2):
                for p in range(2):
                    for q in range(0, count, 8):
                        out[p, 0, pl.ds((2 * q + e) * 8 + r, 8, stride=16), :] = s4[
                            pair, e, p * count + q : p * count + q + 8, i * LANES : (i + 1) * LANES
                        ]

    steps = [
        first_dots,
        first_twist,
        lambda pair: lane_dots(pair, y1, middle, s2),
        respond,
        lambda pair: lane_dots(pair, y2, back, s3),
        back_twist,
        last_dots,
        store,
    ]
    streams = [[(step, pair) for pair in range(k, rows // 2, 2) for step in range(8)] for k in range(2)]
    for t in range(len(streams[0]) + 1):
        now = [s[t - k] for k, s in enumerate(streams) if 0 <= t - k < len(s)]
        for step, pair in sorted(now, key=lambda job: job[0] % 2):
            steps[step](pair)


def focus(blocks, bases, own, other, ramps, first, t, scalars, held, rows, row0, total, slow, out_slow):
    slots, pieces = rows // 2, len(own)
    hbm = pl.BlockSpec(memory_space=pltpu.HBM)
    sm = pl.BlockSpec(memory_space=pltpu.SMEM)
    tile = row0 // 8
    whole = pl.BlockSpec((2, 1, out_slow * 8, LANES), lambda i: (0, tile, 0, 0))

    def full(a):
        return pl.BlockSpec(a.shape, lambda i: (0,) * a.ndim)

    operands = [*own, *other, *ramps, first, *t]
    aliases = {}
    if held is None:
        held = jnp.zeros((8, LANES), jnp.float32)
    else:
        aliases = {1 + len(blocks) + len(operands): 0}
    return pl.pallas_call(
        functools.partial(focus_kernel, tuple(bases), pieces, rows, row0, slow, out_slow),
        grid=(1,),
        in_specs=[sm] + [full(a) for a in blocks + operands] + [hbm],
        out_specs=whole,
        out_shape=jax.ShapeDtypeStruct((2, total // 8, out_slow * 8, LANES), jnp.float32),
        scratch_shapes=[
            pltpu.VMEM((slots, 2, slow, 2 * LANES), jnp.float32),
            pltpu.VMEM((slots, 2, slow, 4 * LANES), jnp.bfloat16),
            pltpu.VMEM((slots, 2 * slow, 2 * LANES), jnp.float32),
            pltpu.VMEM((slots, 2, slow, 4 * LANES), jnp.bfloat16),
            pltpu.VMEM((slots, 2 * slow, 2 * LANES), jnp.float32),
            pltpu.VMEM((slots, 2, 2, slow, 2 * LANES), jnp.bfloat16),
            pltpu.VMEM((slots, 2, out_slow, 2 * LANES), jnp.float32),
            pltpu.VMEM((2, slow, total), jnp.float32),
            pltpu.VMEM((2, pieces * own[0].shape[0], *own[0].shape[1:]), jnp.bfloat16),
        ],
        input_output_aliases=aliases,
        compiler_params=pltpu.CompilerParams(vmem_limit_bytes=24 * 1024 * 1024),
        cost_estimate=pl.CostEstimate(flops=3 * 10**9, bytes_accessed=8 * 10**6, transcendentals=0),
    )(scalars, *blocks, *operands, held)


def swap(value, axis, flip):
    size = lax.axis_size(axis)
    return lax.ppermute(value, axis, [(a, a ^ flip) for a in range(size)])


def per_device(echoes, filters, slab_index, shifts):
    turns, strips, zones = lax.axis_size("turn"), lax.axis_size("strip"), lax.axis_size("blk")
    turn, strip, zone = lax.axis_index("turn"), lax.axis_index("strip"), lax.axis_index("blk")
    sources = turns * strips
    length = echoes.shape[2] * sources
    slow = length // LANES
    total = slab_index.shape[0]
    out_slow = slow // strips
    per_zone = filters.shape[1]
    width = slow // sources
    me = turn * strips + strip
    core = turn % 2
    ids = jnp.stack([turn, core, me]).astype(jnp.int32)
    t = [jnp.asarray(a) for a in tables(length, sources, length // strips)]

    jobs = [[(0, 0, total), (1, 0, total)], []]
    starts = [sum(CHUNKS[:k]) for k in range(len(CHUNKS))]
    for k, rows in enumerate(CHUNKS):
        jobs[min(k, 1)] += [(flip, starts[k], rows) for flip in range(2, turns)]
    sent = pack(ids, echoes, jobs[0], total, 32 * 10**6)
    more = pack(ids, echoes, jobs[1], total, 4 * 10**6)
    half = turn_filters(ids, filters)
    first = order_tables(ids, *t, width)
    held = {}
    for (flip, start, rows), block in zip(jobs[0] + jobs[1], [*sent, *more]):
        if flip:
            block = swap(block, "turn", flip)
        for ds in range(strips):
            mine = swap(block, "strip", ds) if ds else block
            held[flip * strips + ds, start] = mine

    own = [half] + [swap(half, "blk", d) for d in range(1, zones)]
    other = [swap(piece, "turn", 1) for piece in own]
    local_slab = (slab_index // per_zone ^ zone) * per_zone + slab_index % per_zone

    c = jnp.arange(slow, dtype=jnp.int32)[None, :]
    offset = (shifts + (strips - strip) * (length // strips)) % length
    c_angle = (offset[:, None] * c % length).astype(jnp.float32) * (2.0 * math.pi / length)
    d = jnp.arange(LANES, dtype=jnp.int32)[None, :]
    d_angle = (d * (shifts[:, None] % LANES) % LANES).astype(jnp.float32) * (2.0 * math.pi / LANES)
    ramps = (jnp.cos(c_angle), -jnp.sin(c_angle), jnp.cos(d_angle), -jnp.sin(d_angle))
    scalars = jnp.concatenate([core[None].astype(jnp.int32), local_slab])

    image = None
    for start, rows in zip(starts, CHUNKS):
        blocks, bases = [], []
        for slot in range(sources):
            whole = slot // strips < 2
            blocks.append(held[slot, 0 if whole else start])
            bases.append(start if whole else 0)
        image = focus(blocks, bases, own, other, ramps, first, t, scalars, image, rows, start, total, slow, out_slow)
    image = image.reshape(2, total // 8, out_slow, 8, LANES).transpose(0, 1, 3, 2, 4)
    return image.reshape(2, total, out_slow * LANES)


def solution(mesh):
    in_specs = (
        P(None, "blk", ("turn", "strip")),
        P(None, "blk", None),
        P(("blk", "turn")),
        P(("blk", "turn")),
    )
    out_specs = P(None, ("blk", "turn"), "strip")

    return jax.shard_map(per_device, mesh=mesh, in_specs=in_specs, out_specs=out_specs, check_vma=False)
```

```python
import functools
import math

import jax
import jax.numpy as jnp
import numpy as np
from jax import lax
from jax.experimental import pallas as pl
from jax.experimental.pallas import tpu as pltpu
from jax.sharding import PartitionSpec as P


LANES = 128
CHUNKS = (8, 8)


def hi_lo(table):
    high = table.astype(jnp.bfloat16)
    low = (table - high.astype(np.float64)).astype(jnp.bfloat16)
    return high, low


def block_matrix(phase, sign):
    cos, sin = np.cos(phase), sign * np.sin(phase)
    return np.concatenate([np.concatenate([cos, -sin], 1), np.concatenate([sin, cos], 1)], 0)


@functools.lru_cache(maxsize=None)
def tables(length, sources, out_len):
    slow = length // LANES
    half = slow // 2
    part = half // sources
    out_half = out_len // LANES // 2
    q = np.arange(slow)
    c = np.arange(half)
    lane = np.arange(LANES)
    lane_phase = 2 * np.pi * (lane[:, None] * lane[None, :] % LANES) / LANES
    twist = 2 * np.pi * (q[:, None] * lane[None, :]) / length
    first, last = [], []
    for parity in range(2):
        index = 2 * c + parity
        table = block_matrix(2 * np.pi * (c[:, None] * index[None, :] % slow) / slow, -1.0)
        table = table.reshape(slow, 2, sources, part).transpose(0, 2, 1, 3).reshape(slow, slow)
        first.append(np.stack(hi_lo(table)))
        table = block_matrix(2 * np.pi * (index[:out_half, None] * c[None, :] % slow) / slow, 1.0) / length
        last.append(np.stack(hi_lo(table)))
    middle = np.stack(hi_lo(block_matrix(lane_phase, -1.0).T))
    back = np.stack(hi_lo(block_matrix(lane_phase, 1.0).T))
    parts = [np.stack(first), middle, back, np.stack(last)]
    dots = np.concatenate([a.reshape(-1, a.shape[-1]) for a in parts], 0)
    return dots, np.stack([np.cos(twist), np.sin(twist)]).astype(np.float32)


def split(value):
    high = value.astype(jnp.bfloat16)
    return high, (value - high.astype(jnp.float32)).astype(jnp.bfloat16)


def dot(a, b):
    return jnp.dot(a, b, preferred_element_type=jnp.float32)


def pack_kernel(jobs, total, part, echoes, *refs):
    turn, outs, spread = lax.axis_index("turn"), refs[:-1], refs[-1]
    for k, (flip, row0, rows) in enumerate(jobs):
        for row in range(0, rows, 8):
            start = pl.multiple_of((turn ^ flip) * total + row0 + row, 8)
            for p in range(2):
                block = echoes[p, pl.ds(start, 8), :].astype(jnp.float32)
                for q in range(part):
                    spread[k, row // 8, p, q * 8 : (q + 1) * 8] = block[:, q * LANES : (q + 1) * LANES]
    for k, (flip, row0, rows) in enumerate(jobs):
        for row in range(rows):
            for p in range(2):
                for e in range(2):
                    start = e * 8 + row % 8
                    picked = spread[k, row // 8, p, pl.ds(start, part // 2, stride=16), :]
                    outs[k][p, row, e] = picked.astype(jnp.bfloat16)


def pack(echoes, jobs, total, cost):
    part = echoes.shape[2] // LANES
    vm = pl.BlockSpec(memory_space=pltpu.VMEM)
    tiles = max(rows for _, _, rows in jobs) // 8
    return pl.pallas_call(
        functools.partial(pack_kernel, tuple(jobs), total, part),
        in_specs=[vm],
        out_specs=[vm] * len(jobs),
        out_shape=[jax.ShapeDtypeStruct((2, rows, 2, part // 2, LANES), jnp.bfloat16) for _, _, rows in jobs],
        scratch_shapes=[pltpu.VMEM((len(jobs), tiles, 2, part * 8, LANES), jnp.float32)],
        compiler_params=pltpu.CompilerParams(vmem_limit_bytes=12 * 1024 * 1024),
        cost_estimate=pl.CostEstimate(flops=10**6, bytes_accessed=cost, transcendentals=0),
    )(echoes)


def order_kernel(width, strips, dots, twist, out):
    me = lax.axis_index("turn") * strips + lax.axis_index("strip")
    size = dots.shape[1]
    row_ids = lax.broadcasted_iota(jnp.int32, (size, size), 0)
    col_ids = lax.broadcasted_iota(jnp.int32, (size, size), 1)
    order = jnp.where(row_ids == (col_ids ^ (me * width)), 1.0, 0.0).astype(jnp.bfloat16)
    out[...] = dot(dots[: 4 * size], order).astype(jnp.bfloat16)


def order_tables(dots, twist, width, strips):
    vm = pl.BlockSpec(memory_space=pltpu.VMEM)
    size = dots.shape[1]
    return pl.pallas_call(
        functools.partial(order_kernel, width, strips),
        in_specs=[vm, vm],
        out_specs=vm,
        out_shape=jax.ShapeDtypeStruct((4 * size, size), jnp.bfloat16),
        compiler_params=pltpu.CompilerParams(vmem_limit_bytes=8 * 1024 * 1024),
        cost_estimate=pl.CostEstimate(flops=10**6, bytes_accessed=4 * 10**6, transcendentals=0),
    )(dots, twist)


def turn_kernel(filters, out, turned):
    core = lax.axis_index("turn") % 2
    slabs = filters.shape[1]
    for p in range(2):
        for d in range(LANES):
            at = pl.multiple_of((2 * d + core) * LANES, LANES)
            lanes = filters[p, :, pl.ds(at, LANES)].astype(jnp.float32)
            for slab in range(slabs):
                turned[slab, p, d : d + 1, :] = lanes[slab : slab + 1]
    for p in range(2):
        for slab in range(slabs):
            out[slab, p] = turned[slab, p].T.astype(jnp.bfloat16)


def turn_filters(filters):
    vm = pl.BlockSpec(memory_space=pltpu.VMEM)
    shape = (filters.shape[1], 2, LANES, LANES)
    return pl.pallas_call(
        turn_kernel,
        in_specs=[vm],
        out_specs=vm,
        out_shape=jax.ShapeDtypeStruct(shape, jnp.bfloat16),
        scratch_shapes=[pltpu.VMEM(shape, jnp.float32)],
        compiler_params=pltpu.CompilerParams(vmem_limit_bytes=4 * 1024 * 1024),
        cost_estimate=pl.CostEstimate(flops=10**6, bytes_accessed=16 * 10**6, transcendentals=0),
    )(filters)


def focus_kernel(bases, pieces, earlier, rows, row0, slow, out_slow, *refs):
    sources = len(bases)
    slabs, blocks = refs[0], refs[1 : 1 + sources]
    own = refs[1 + sources : 1 + sources + pieces]
    other = refs[1 + sources + pieces : 1 + sources + 2 * pieces]
    slow_cos, slow_sin, fast_cos, fast_sin, first_dots_ref, dots, twist = refs[1 + sources + 2 * pieces :][:7]
    rest = refs[8 + sources + 2 * pieces :]
    images, out = rest[:earlier], rest[earlier]
    s1, y1, s2, y2, s3, y3, s4, slow_ramp, filt, slab_ids, slab_sem = rest[earlier + 1 :][:11]
    fetch = pltpu.make_async_copy(slabs, slab_ids, slab_sem)
    fetch.start()
    tile = out
    writes = []
    if earlier:
        tile, write_sem = rest[earlier + 12 :]
        for k, source in enumerate((*images, tile)):
            for p in range(2):
                writes.append(pltpu.make_async_copy(source.at[p], out.at[p, k], write_sem.at[2 * k + p]))
        for write in writes[:-2]:
            write.start()
    core = lax.axis_index("turn") % 2
    per_zone = own[0].shape[0]
    for k in range(pieces):
        filt[core, k * per_zone : (k + 1) * per_zone] = own[k][...]
        filt[1 - core, k * per_zone : (k + 1) * per_zone] = other[k][...]
    slow_ramp[0] = slow_cos[...].T
    slow_ramp[1] = slow_sin[...].T
    half = slow // 2
    wide = 2 * LANES
    first = [[first_dots_ref.at[pl.ds((2 * e + k) * slow, slow)] for k in range(2)] for e in range(2)]
    base = 4 * slow
    middle = [dots.at[pl.ds(base + k * wide, wide)] for k in range(2)]
    back = [dots.at[pl.ds(base + (2 + k) * wide, wide)] for k in range(2)]
    base += 4 * wide
    last = [[dots.at[pl.ds(base + (2 * e + k) * out_slow, out_slow)] for k in range(2)] for e in range(2)]

    def first_dots(pair):
        for e in range(2):
            data = jnp.concatenate(
                [
                    jnp.concatenate([block[p, base + r, e] for block, base in zip(blocks, bases) for p in range(2)], 0)
                    for r in (2 * pair, 2 * pair + 1)
                ],
                1,
            )
            s1[pair, e] = dot(first[e][0][...], data) + dot(first[e][1][...], data)

    def first_twist(pair):
        for i in range(2):
            lanes = slice(i * LANES, (i + 1) * LANES)
            for part in range(2):
                rows_c = slice(part * half, (part + 1) * half)
                even_re, even_im = s1[pair, 0, :half, lanes], s1[pair, 0, half:, lanes]
                odd_re, odd_im = s1[pair, 1, :half, lanes], s1[pair, 1, half:, lanes]
                if part == 0:
                    re, im = even_re + odd_re, even_im + odd_im
                else:
                    re, im = even_re - odd_re, even_im - odd_im
                tw_re, tw_im = twist[0, rows_c], twist[1, rows_c]
                (rh, rl), (ih, il) = split(re * tw_re + im * tw_im), split(im * tw_re - re * tw_im)
                y1[pair, i, rows_c] = jnp.concatenate([rh, ih, rl, il], 1)

    def lane_dots(pair, source, table, target):
        mix = source[pair].reshape(2 * slow, 2 * wide)
        target[pair] = (
            dot(mix[:, :wide], table[0][...]) + dot(mix[:, wide:], table[0][...]) + dot(mix[:, :wide], table[1][...])
        )

    def respond(pair):
        for i in range(2):
            r = row0 + 2 * pair + i
            slab = slab_ids[r]
            v_re, v_im = fast_cos[r : r + 1], fast_sin[r : r + 1]
            for part in range(2):
                rows_s = slice(i * slow + part * half, i * slow + (part + 1) * half)
                re, im = s2[pair, rows_s, :LANES], s2[pair, rows_s, LANES:]
                h_re = filt[part, slab, 0].astype(jnp.float32)
                h_im = filt[part, slab, 1].astype(jnp.float32)
                re, im = re * h_re - im * h_im, re * h_im + im * h_re
                (rh, rl), (ih, il) = split(re * v_re - im * v_im), split(re * v_im + im * v_re)
                y2[pair, i, part * half : (part + 1) * half] = jnp.concatenate([rh, ih, rl, il], 1)

    def back_twist(pair):
        for i in range(2):
            r = row0 + 2 * pair + i
            lanes = slice(i * LANES, (i + 1) * LANES)
            parts = []
            for part in range(2):
                rows_c = slice(part * half, (part + 1) * half)
                rows_s = slice(i * slow + part * half, i * slow + (part + 1) * half)
                re, im = s3[pair, rows_s, :LANES], s3[pair, rows_s, LANES:]
                tw_re, tw_im = twist[0, rows_c], twist[1, rows_c]
                re, im = re * tw_re - im * tw_im, re * tw_im + im * tw_re
                u_re, u_im = slow_ramp[0, rows_c, r : r + 1], slow_ramp[1, rows_c, r : r + 1]
                parts.append((re * u_re - im * u_im, re * u_im + im * u_re))
            (a_re, a_im), (b_re, b_im) = parts
            for e, (re, im) in enumerate(((a_re + b_re, a_im + b_im), (a_re - b_re, a_im - b_im))):
                (rh, rl), (ih, il) = split(re), split(im)
                y3[pair, e, 0, :, lanes] = jnp.concatenate([rh, ih], 0)
                y3[pair, e, 1, :, lanes] = jnp.concatenate([rl, il], 0)

    def last_dots(pair):
        for e in range(2):
            high, low = y3[pair, e, 0], y3[pair, e, 1]
            s4[pair, e] = (
                dot(last[e][0][...], high) + dot(last[e][1][...], high) + dot(last[e][0][...], low)
            )

    def store(pair):
        count = out_slow // 2
        for i in range(2):
            r = (row0 + 2 * pair + i) % 8
            for e in range(2):
                for p in range(2):
                    for q in range(0, count, 8):
                        tile[p, pl.ds((2 * q + e) * 8 + r, 8, stride=16), :] = s4[
                            pair, e, p * count + q : p * count + q + 8, i * LANES : (i + 1) * LANES
                        ]

    steps = [
        first_dots,
        first_twist,
        lambda pair: lane_dots(pair, y1, middle, s2),
        respond,
        lambda pair: lane_dots(pair, y2, back, s3),
        back_twist,
        last_dots,
        store,
    ]
    streams = [[(step, pair) for pair in range(k, rows // 2, 2) for step in range(8)] for k in range(2)]
    fetch.wait()
    for t in range(len(streams[0]) + 1):
        now = [s[t - k] for k, s in enumerate(streams) if 0 <= t - k < len(s)]
        for step, pair in sorted(now, key=lambda job: job[0] % 2):
            steps[step](pair)
    for write in writes[-2:]:
        write.start()
    for write in writes:
        write.wait()


def focus(blocks, bases, own, other, ramps, first, t, slabs, images, rows, row0, total, slow, out_slow, final):
    slots, pieces = rows // 2, len(own)

    def full(a):
        return pl.BlockSpec(a.shape, lambda i: (0,) * a.ndim)

    image = (2, out_slow * 8, LANES)
    shape = (2, total // 8, *image[1:]) if final else image
    operands = [slabs, *blocks, *own, *other, *ramps, first, *t, *images]
    extra = [pltpu.VMEM(image, jnp.float32), pltpu.SemaphoreType.DMA((total // 4,))] if final else []
    return pl.pallas_call(
        functools.partial(focus_kernel, tuple(bases), pieces, len(images), rows, row0, slow, out_slow),
        grid=(1,),
        in_specs=[full(a) for a in operands],
        out_specs=pl.BlockSpec(memory_space=pl.ANY) if final else pl.BlockSpec(image, lambda i: (0, 0, 0)),
        out_shape=jax.ShapeDtypeStruct(shape, jnp.float32),
        scratch_shapes=[
            pltpu.VMEM((slots, 2, slow, 2 * LANES), jnp.float32),
            pltpu.VMEM((slots, 2, slow, 4 * LANES), jnp.bfloat16),
            pltpu.VMEM((slots, 2 * slow, 2 * LANES), jnp.float32),
            pltpu.VMEM((slots, 2, slow, 4 * LANES), jnp.bfloat16),
            pltpu.VMEM((slots, 2 * slow, 2 * LANES), jnp.float32),
            pltpu.VMEM((slots, 2, 2, slow, 2 * LANES), jnp.bfloat16),
            pltpu.VMEM((slots, 2, out_slow, 2 * LANES), jnp.float32),
            pltpu.VMEM((2, slow, total), jnp.float32),
            pltpu.VMEM((2, pieces * own[0].shape[0], *own[0].shape[1:]), jnp.bfloat16),
            pltpu.SMEM(slabs.shape, jnp.int32),
            pltpu.SemaphoreType.DMA,
            *extra,
        ],
        compiler_params=pltpu.CompilerParams(vmem_limit_bytes=28 * 1024 * 1024),
        cost_estimate=pl.CostEstimate(flops=3 * 10**9, bytes_accessed=8 * 10**6, transcendentals=0),
    )(*operands)


def swap(value, axis, flip):
    size = lax.axis_size(axis)
    return lax.ppermute(value, axis, [(a, a ^ flip) for a in range(size)])


def per_device(echoes, filters, slab_index, shifts):
    turns, strips, zones = lax.axis_size("turn"), lax.axis_size("strip"), lax.axis_size("blk")
    strip, zone = lax.axis_index("strip"), lax.axis_index("blk")
    sources = turns * strips
    length = echoes.shape[2] * sources
    slow = length // LANES
    total = slab_index.shape[0]
    out_slow = slow // strips
    per_zone = filters.shape[1]
    width = slow // sources
    behind = (strips - strip) * (length // strips)
    echoes, zone, behind = lax.optimization_barrier((echoes, zone, behind))
    t = [jnp.asarray(a) for a in tables(length, sources, length // strips)]

    jobs = [[(0, 0, total), (1, 0, total)], []]
    starts = [sum(CHUNKS[:k]) for k in range(len(CHUNKS))]
    for k, rows in enumerate(CHUNKS):
        jobs[min(k, 1)] += [(flip, starts[k], rows) for flip in range(2, turns)]
    sent = pack(echoes, jobs[0], total, 32 * 10**6)
    more = pack(echoes, jobs[1], total, 4 * 10**6)
    half = turn_filters(filters)
    first = order_tables(*t, width, strips)
    held = {}
    for (flip, start, rows), block in zip(jobs[0] + jobs[1], [*sent, *more]):
        if flip:
            block = swap(block, "turn", flip)
        for ds in range(strips):
            mine = swap(block, "strip", ds) if ds else block
            held[flip * strips + ds, start] = mine

    own = [half] + [swap(half, "blk", d) for d in range(1, zones)]
    other = [swap(piece, "turn", 1) for piece in own]
    local_slab = (slab_index // per_zone ^ zone) * per_zone + slab_index % per_zone

    c = jnp.arange(slow, dtype=jnp.int32)[None, :]
    offset = (shifts + behind) & (length - 1)
    c_angle = (offset[:, None] * c & (length - 1)).astype(jnp.float32) * (2.0 * math.pi / length)
    d = jnp.arange(LANES, dtype=jnp.int32)[None, :]
    d_angle = (d * shifts[:, None] & (LANES - 1)).astype(jnp.float32) * (2.0 * math.pi / LANES)
    ramps = (jnp.cos(c_angle), -jnp.sin(c_angle), jnp.cos(d_angle), -jnp.sin(d_angle))

    images = []
    for k, (start, rows) in enumerate(zip(starts, CHUNKS)):
        blocks, bases = [], []
        for slot in range(sources):
            whole = slot // strips < 2
            blocks.append(held[slot, 0 if whole else start])
            bases.append(start if whole else 0)
        final = k == len(CHUNKS) - 1
        image = focus(
            blocks, bases, own, other, ramps, first, t, local_slab, images, rows, start, total, slow, out_slow, final
        )
        images.append(image)
    image = image.reshape(2, total // 8, out_slow, 8, LANES).transpose(0, 1, 3, 2, 4)
    return image.reshape(2, total, out_slow * LANES)


def solution(mesh):
    in_specs = (
        P(None, "blk", ("turn", "strip")),
        P(None, "blk", None),
        P(("blk", "turn")),
        P(("blk", "turn")),
    )
    out_specs = P(None, ("blk", "turn"), "strip")

    return jax.shard_map(per_device, mesh=mesh, in_specs=in_specs, out_specs=out_specs, check_vma=False)
```

```python
import functools
import math

import jax
import jax.numpy as jnp
import numpy as np
from jax import lax
from jax.experimental import pallas as pl
from jax.experimental.pallas import tpu as pltpu
from jax.sharding import PartitionSpec as P


LANES = 128
CHUNKS = (8, 8)


def hi_lo(table):
    high = table.astype(jnp.bfloat16)
    low = (table - high.astype(np.float64)).astype(jnp.bfloat16)
    return high, low


def block_matrix(phase, sign):
    cos, sin = np.cos(phase), sign * np.sin(phase)
    return np.concatenate([np.concatenate([cos, -sin], 1), np.concatenate([sin, cos], 1)], 0)


@functools.lru_cache(maxsize=None)
def tables(length, sources, out_len):
    slow = length // LANES
    half = slow // 2
    part = half // sources
    out_half = out_len // LANES // 2
    q = np.arange(slow)
    c = np.arange(half)
    lane = np.arange(LANES)
    lane_phase = 2 * np.pi * (lane[:, None] * lane[None, :] % LANES) / LANES
    twist = 2 * np.pi * (q[:, None] * lane[None, :]) / length
    first, last = [], []
    for parity in range(2):
        index = 2 * c + parity
        table = block_matrix(2 * np.pi * (c[:, None] * index[None, :] % slow) / slow, -1.0)
        table = table.reshape(slow, 2, sources, part).transpose(0, 2, 1, 3).reshape(slow, slow)
        first.append(np.stack(hi_lo(table)))
        table = block_matrix(2 * np.pi * (index[:out_half, None] * c[None, :] % slow) / slow, 1.0) / length
        last.append(np.stack(hi_lo(table)))
    middle = np.stack(hi_lo(block_matrix(lane_phase, -1.0).T))
    back = np.stack(hi_lo(block_matrix(lane_phase, 1.0).T))
    parts = [np.stack(first), middle, back, np.stack(last)]
    left = np.concatenate([np.cos(twist), np.sin(twist)], 1).astype(np.float32)
    for _ in range(3):
        parts.append(left.astype(jnp.bfloat16))
        left = left - parts[-1].astype(np.float32)
    return np.concatenate([a.reshape(-1, a.shape[-1]) for a in parts], 0)


def split(value):
    high = value.astype(jnp.bfloat16)
    return high, (value - high.astype(jnp.float32)).astype(jnp.bfloat16)


def dot(a, b):
    return jnp.dot(a, b, preferred_element_type=jnp.float32)


def pack_kernel(jobs, total, part, echoes, *refs):
    turn, outs, spread = lax.axis_index("turn"), refs[:-1], refs[-1]
    for k, (flip, row0, rows) in enumerate(jobs):
        for row in range(0, rows, 8):
            start = pl.multiple_of((turn ^ flip) * total + row0 + row, 8)
            for p in range(2):
                block = echoes[p, pl.ds(start, 8), :].astype(jnp.float32)
                for q in range(part):
                    spread[k, row // 8, p, q * 8 : (q + 1) * 8] = block[:, q * LANES : (q + 1) * LANES]
    for k, (flip, row0, rows) in enumerate(jobs):
        for row in range(rows):
            for p in range(2):
                for e in range(2):
                    start = e * 8 + row % 8
                    picked = spread[k, row // 8, p, pl.ds(start, part // 2, stride=16), :]
                    outs[k][p, row, e] = picked.astype(jnp.bfloat16)


def pack(echoes, jobs, total, cost):
    part = echoes.shape[2] // LANES
    vm = pl.BlockSpec(memory_space=pltpu.VMEM)
    tiles = max(rows for _, _, rows in jobs) // 8
    return pl.pallas_call(
        functools.partial(pack_kernel, tuple(jobs), total, part),
        in_specs=[vm],
        out_specs=[vm] * len(jobs),
        out_shape=[jax.ShapeDtypeStruct((2, rows, 2, part // 2, LANES), jnp.bfloat16) for _, _, rows in jobs],
        scratch_shapes=[pltpu.VMEM((len(jobs), tiles, 2, part * 8, LANES), jnp.float32)],
        compiler_params=pltpu.CompilerParams(vmem_limit_bytes=12 * 1024 * 1024),
        cost_estimate=pl.CostEstimate(flops=10**6, bytes_accessed=cost, transcendentals=0),
    )(echoes)


def order_kernel(width, strips, slow, dots, out, twist):
    me = lax.axis_index("turn") * strips + lax.axis_index("strip")
    size = dots.shape[1]
    row_ids = lax.broadcasted_iota(jnp.int32, (size, size), 0)
    col_ids = lax.broadcasted_iota(jnp.int32, (size, size), 1)
    order = jnp.where(row_ids == (col_ids ^ (me * width)), 1.0, 0.0).astype(jnp.bfloat16)
    out[...] = dot(dots[: 4 * size], order).astype(jnp.bfloat16)
    base = dots.shape[0] - 3 * slow
    terms = [dots[base + k * slow : base + (k + 1) * slow].astype(jnp.float32) for k in range(3)]
    twist[...] = terms[0] + terms[1] + terms[2]


def order_tables(dots, width, strips, slow):
    vm = pl.BlockSpec(memory_space=pltpu.VMEM)
    size = dots.shape[1]
    return pl.pallas_call(
        functools.partial(order_kernel, width, strips, slow),
        in_specs=[vm],
        out_specs=[vm, vm],
        out_shape=[
            jax.ShapeDtypeStruct((4 * size, size), jnp.bfloat16),
            jax.ShapeDtypeStruct((slow, 2 * LANES), jnp.float32),
        ],
        compiler_params=pltpu.CompilerParams(vmem_limit_bytes=8 * 1024 * 1024),
        cost_estimate=pl.CostEstimate(flops=10**6, bytes_accessed=2 * 10**6, transcendentals=0),
    )(dots)


def turn_kernel(filters, out, turned):
    core = lax.axis_index("turn") % 2
    slabs = filters.shape[1]
    for p in range(2):
        for d in range(LANES):
            at = pl.multiple_of((2 * d + core) * LANES, LANES)
            lanes = filters[p, :, pl.ds(at, LANES)].astype(jnp.float32)
            for slab in range(slabs):
                turned[slab, p, d : d + 1, :] = lanes[slab : slab + 1]
    for p in range(2):
        for slab in range(slabs):
            out[slab, p] = turned[slab, p].T.astype(jnp.bfloat16)


def turn_filters(filters):
    vm = pl.BlockSpec(memory_space=pltpu.VMEM)
    shape = (filters.shape[1], 2, LANES, LANES)
    return pl.pallas_call(
        turn_kernel,
        in_specs=[vm],
        out_specs=vm,
        out_shape=jax.ShapeDtypeStruct(shape, jnp.bfloat16),
        scratch_shapes=[pltpu.VMEM(shape, jnp.float32)],
        compiler_params=pltpu.CompilerParams(vmem_limit_bytes=4 * 1024 * 1024),
        cost_estimate=pl.CostEstimate(flops=10**6, bytes_accessed=2 * 10**6, transcendentals=0),
    )(filters)


def focus_kernel(bases, pieces, earlier, rows, row0, slow, out_slow, *refs):
    sources = len(bases)
    slabs, blocks = refs[0], refs[1 : 1 + sources]
    own = refs[1 + sources : 1 + sources + pieces]
    other = refs[1 + sources + pieces : 1 + sources + 2 * pieces]
    slow_cos, slow_sin, fast_cos, fast_sin, first_dots_ref, dots, twist = refs[1 + sources + 2 * pieces :][:7]
    rest = refs[8 + sources + 2 * pieces :]
    images, out = rest[:earlier], rest[earlier]
    s1, y1, s2, y2, s3, y3, s4, slow_ramp, filt, slab_ids, slab_sem = rest[earlier + 1 :][:11]
    fetch = pltpu.make_async_copy(slabs, slab_ids, slab_sem)
    fetch.start()
    tile = out
    writes = []
    if earlier:
        tile, write_sem = rest[earlier + 12 :]
        for k, source in enumerate((*images, tile)):
            for p in range(2):
                writes.append(pltpu.make_async_copy(source.at[p], out.at[p, k], write_sem.at[2 * k + p]))
        for write in writes[:-2]:
            write.start()
    core = lax.axis_index("turn") % 2
    per_zone = own[0].shape[0]
    for k in range(pieces):
        filt[core, k * per_zone : (k + 1) * per_zone] = own[k][...]
        filt[1 - core, k * per_zone : (k + 1) * per_zone] = other[k][...]
    slow_ramp[0] = slow_cos[...].T
    slow_ramp[1] = slow_sin[...].T
    half = slow // 2
    wide = 2 * LANES
    first = [[first_dots_ref.at[pl.ds((2 * e + k) * slow, slow)] for k in range(2)] for e in range(2)]
    base = 4 * slow
    middle = [dots.at[pl.ds(base + k * wide, wide)] for k in range(2)]
    back = [dots.at[pl.ds(base + (2 + k) * wide, wide)] for k in range(2)]
    base += 4 * wide
    last = [[dots.at[pl.ds(base + (2 * e + k) * out_slow, out_slow)] for k in range(2)] for e in range(2)]

    def first_dots(pair):
        for e in range(2):
            data = jnp.concatenate(
                [
                    jnp.concatenate([block[p, base + r, e] for block, base in zip(blocks, bases) for p in range(2)], 0)
                    for r in (2 * pair, 2 * pair + 1)
                ],
                1,
            )
            s1[pair, e] = dot(first[e][0][...], data) + dot(first[e][1][...], data)

    def first_twist(pair):
        for i in range(2):
            lanes = slice(i * LANES, (i + 1) * LANES)
            for part in range(2):
                rows_c = slice(part * half, (part + 1) * half)
                even_re, even_im = s1[pair, 0, :half, lanes], s1[pair, 0, half:, lanes]
                odd_re, odd_im = s1[pair, 1, :half, lanes], s1[pair, 1, half:, lanes]
                if part == 0:
                    re, im = even_re + odd_re, even_im + odd_im
                else:
                    re, im = even_re - odd_re, even_im - odd_im
                tw_re, tw_im = twist[rows_c, :LANES], twist[rows_c, LANES:]
                (rh, rl), (ih, il) = split(re * tw_re + im * tw_im), split(im * tw_re - re * tw_im)
                y1[pair, i, rows_c] = jnp.concatenate([rh, ih, rl, il], 1)

    def lane_dots(pair, source, table, target):
        mix = source[pair].reshape(2 * slow, 2 * wide)
        target[pair] = (
            dot(mix[:, :wide], table[0][...]) + dot(mix[:, wide:], table[0][...]) + dot(mix[:, :wide], table[1][...])
        )

    def respond(pair):
        for i in range(2):
            r = row0 + 2 * pair + i
            slab = slab_ids[r]
            v_re, v_im = fast_cos[r : r + 1], fast_sin[r : r + 1]
            for part in range(2):
                rows_s = slice(i * slow + part * half, i * slow + (part + 1) * half)
                re, im = s2[pair, rows_s, :LANES], s2[pair, rows_s, LANES:]
                h_re = filt[part, slab, 0].astype(jnp.float32)
                h_im = filt[part, slab, 1].astype(jnp.float32)
                re, im = re * h_re - im * h_im, re * h_im + im * h_re
                (rh, rl), (ih, il) = split(re * v_re - im * v_im), split(re * v_im + im * v_re)
                y2[pair, i, part * half : (part + 1) * half] = jnp.concatenate([rh, ih, rl, il], 1)

    def back_twist(pair):
        for i in range(2):
            r = row0 + 2 * pair + i
            lanes = slice(i * LANES, (i + 1) * LANES)
            parts = []
            for part in range(2):
                rows_c = slice(part * half, (part + 1) * half)
                rows_s = slice(i * slow + part * half, i * slow + (part + 1) * half)
                re, im = s3[pair, rows_s, :LANES], s3[pair, rows_s, LANES:]
                tw_re, tw_im = twist[rows_c, :LANES], twist[rows_c, LANES:]
                re, im = re * tw_re - im * tw_im, re * tw_im + im * tw_re
                u_re, u_im = slow_ramp[0, rows_c, r : r + 1], slow_ramp[1, rows_c, r : r + 1]
                parts.append((re * u_re - im * u_im, re * u_im + im * u_re))
            (a_re, a_im), (b_re, b_im) = parts
            for e, (re, im) in enumerate(((a_re + b_re, a_im + b_im), (a_re - b_re, a_im - b_im))):
                (rh, rl), (ih, il) = split(re), split(im)
                y3[pair, e, 0, :, lanes] = jnp.concatenate([rh, ih], 0)
                y3[pair, e, 1, :, lanes] = jnp.concatenate([rl, il], 0)

    def last_dots(pair):
        for e in range(2):
            high, low = y3[pair, e, 0], y3[pair, e, 1]
            s4[pair, e] = (
                dot(last[e][0][...], high) + dot(last[e][1][...], high) + dot(last[e][0][...], low)
            )

    def store(pair):
        count = out_slow // 2
        for i in range(2):
            r = (row0 + 2 * pair + i) % 8
            for e in range(2):
                for p in range(2):
                    for q in range(0, count, 8):
                        tile[p, pl.ds((2 * q + e) * 8 + r, 8, stride=16), :] = s4[
                            pair, e, p * count + q : p * count + q + 8, i * LANES : (i + 1) * LANES
                        ]

    steps = [
        first_dots,
        first_twist,
        lambda pair: lane_dots(pair, y1, middle, s2),
        respond,
        lambda pair: lane_dots(pair, y2, back, s3),
        back_twist,
        last_dots,
        store,
    ]
    streams = [[(step, pair) for pair in range(k, rows // 2, 2) for step in range(8)] for k in range(2)]
    fetch.wait()
    for t in range(len(streams[0]) + 1):
        now = [s[t - k] for k, s in enumerate(streams) if 0 <= t - k < len(s)]
        for step, pair in sorted(now, key=lambda job: job[0] % 2):
            steps[step](pair)
    for write in writes[-2:]:
        write.start()
    for write in writes:
        write.wait()


def focus(blocks, bases, own, other, ramps, tables, slabs, images, rows, row0, total, slow, out_slow, final):
    slots, pieces = rows // 2, len(own)

    def full(a):
        return pl.BlockSpec(a.shape, lambda i: (0,) * a.ndim)

    image = (2, out_slow * 8, LANES)
    shape = (2, total // 8, *image[1:]) if final else image
    operands = [slabs, *blocks, *own, *other, *ramps, *tables, *images]
    extra = [pltpu.VMEM(image, jnp.float32), pltpu.SemaphoreType.DMA((total // 4,))] if final else []
    return pl.pallas_call(
        functools.partial(focus_kernel, tuple(bases), pieces, len(images), rows, row0, slow, out_slow),
        grid=(1,),
        in_specs=[full(a) for a in operands],
        out_specs=pl.BlockSpec(memory_space=pl.ANY) if final else pl.BlockSpec(image, lambda i: (0, 0, 0)),
        out_shape=jax.ShapeDtypeStruct(shape, jnp.float32),
        scratch_shapes=[
            pltpu.VMEM((slots, 2, slow, 2 * LANES), jnp.float32),
            pltpu.VMEM((slots, 2, slow, 4 * LANES), jnp.bfloat16),
            pltpu.VMEM((slots, 2 * slow, 2 * LANES), jnp.float32),
            pltpu.VMEM((slots, 2, slow, 4 * LANES), jnp.bfloat16),
            pltpu.VMEM((slots, 2 * slow, 2 * LANES), jnp.float32),
            pltpu.VMEM((slots, 2, 2, slow, 2 * LANES), jnp.bfloat16),
            pltpu.VMEM((slots, 2, out_slow, 2 * LANES), jnp.float32),
            pltpu.VMEM((2, slow, total), jnp.float32),
            pltpu.VMEM((2, pieces * own[0].shape[0], *own[0].shape[1:]), jnp.bfloat16),
            pltpu.SMEM(slabs.shape, jnp.int32),
            pltpu.SemaphoreType.DMA,
            *extra,
        ],
        compiler_params=pltpu.CompilerParams(vmem_limit_bytes=28 * 1024 * 1024),
        cost_estimate=pl.CostEstimate(flops=3 * 10**9, bytes_accessed=8 * 10**6, transcendentals=0),
    )(*operands)


def swap(value, axis, flip):
    size = lax.axis_size(axis)
    return lax.ppermute(value, axis, [(a, a ^ flip) for a in range(size)])


def per_device(echoes, filters, slab_index, shifts):
    turns, strips, zones = lax.axis_size("turn"), lax.axis_size("strip"), lax.axis_size("blk")
    strip, zone = lax.axis_index("strip"), lax.axis_index("blk")
    sources = turns * strips
    length = echoes.shape[2] * sources
    slow = length // LANES
    total = slab_index.shape[0]
    out_slow = slow // strips
    per_zone = filters.shape[1]
    width = slow // sources
    behind = (strips - strip) * (length // strips)
    echoes, zone, behind = lax.optimization_barrier((echoes, zone, behind))
    dots = jnp.asarray(tables(length, sources, length // strips))

    jobs = [[(0, 0, total), (1, 0, total)], []]
    starts = [sum(CHUNKS[:k]) for k in range(len(CHUNKS))]
    for k, rows in enumerate(CHUNKS):
        jobs[min(k, 1)] += [(flip, starts[k], rows) for flip in range(2, turns)]
    sent = pack(echoes, jobs[0], total, 8 * 10**6)
    more = pack(echoes, jobs[1], total, 2 * 10**6)
    half = turn_filters(filters)
    first, twist = order_tables(dots, width, strips, slow)
    held = {}
    for (flip, start, rows), block in zip(jobs[0] + jobs[1], [*sent, *more]):
        if flip:
            block = swap(block, "turn", flip)
        for ds in range(strips):
            mine = swap(block, "strip", ds) if ds else block
            held[flip * strips + ds, start] = mine

    own = [half] + [swap(half, "blk", d) for d in range(1, zones)]
    other = [swap(piece, "turn", 1) for piece in own]
    local_slab = (slab_index // per_zone ^ zone) * per_zone + slab_index % per_zone

    c = jnp.arange(slow, dtype=jnp.int32)[None, :]
    offset = (shifts + behind) & (length - 1)
    c_angle = (offset[:, None] * c & (length - 1)).astype(jnp.float32) * (2.0 * math.pi / length)
    d = jnp.arange(LANES, dtype=jnp.int32)[None, :]
    d_angle = (d * shifts[:, None] & (LANES - 1)).astype(jnp.float32) * (2.0 * math.pi / LANES)
    ramps = (jnp.cos(c_angle), -jnp.sin(c_angle), jnp.cos(d_angle), -jnp.sin(d_angle))

    images = []
    for k, (start, rows) in enumerate(zip(starts, CHUNKS)):
        blocks, bases = [], []
        for slot in range(sources):
            whole = slot // strips < 2
            blocks.append(held[slot, 0 if whole else start])
            bases.append(start if whole else 0)
        final = k == len(CHUNKS) - 1
        image = focus(
            blocks, bases, own, other, ramps, (first, dots, twist), local_slab, images, rows, start, total, slow, out_slow, final
        )
        images.append(image)
    image = image.reshape(2, total // 8, out_slow, 8, LANES).transpose(0, 1, 3, 2, 4)
    return image.reshape(2, total, out_slow * LANES)


def solution(mesh):
    in_specs = (
        P(None, "blk", ("turn", "strip")),
        P(None, "blk", None),
        P(("blk", "turn")),
        P(("blk", "turn")),
    )
    out_specs = P(None, ("blk", "turn"), "strip")

    return jax.shard_map(per_device, mesh=mesh, in_specs=in_specs, out_specs=out_specs, check_vma=False)
```

```python
import functools
import math

import jax
import jax.numpy as jnp
import numpy as np
from jax import lax
from jax.experimental import pallas as pl
from jax.experimental.pallas import tpu as pltpu
from jax.sharding import PartitionSpec as P


LANES = 128
CHUNKS = (8, 8)


def hi_lo(table):
    high = table.astype(jnp.bfloat16)
    low = (table - high.astype(np.float64)).astype(jnp.bfloat16)
    return high, low


def block_matrix(phase, sign):
    cos, sin = np.cos(phase), sign * np.sin(phase)
    return np.concatenate([np.concatenate([cos, -sin], 1), np.concatenate([sin, cos], 1)], 0)


@functools.lru_cache(maxsize=None)
def tables(length, sources, out_len):
    slow = length // LANES
    half = slow // 2
    part = half // sources
    out_half = out_len // LANES // 2
    q = np.arange(slow)
    c = np.arange(half)
    lane = np.arange(LANES)
    lane_phase = 2 * np.pi * (lane[:, None] * lane[None, :] % LANES) / LANES
    twist = 2 * np.pi * (q[:, None] * lane[None, :]) / length
    first, last = [], []
    for parity in range(2):
        index = 2 * c + parity
        table = block_matrix(2 * np.pi * (c[:, None] * index[None, :] % slow) / slow, -1.0)
        table = table.reshape(slow, 2, sources, part).transpose(0, 2, 1, 3).reshape(slow, slow)
        first.append(np.stack(hi_lo(table)))
        table = block_matrix(2 * np.pi * (index[:out_half, None] * c[None, :] % slow) / slow, 1.0) / length
        last.append(np.stack(hi_lo(table)))
    middle = np.stack(hi_lo(block_matrix(lane_phase, -1.0).T))
    back = np.stack(hi_lo(block_matrix(lane_phase, 1.0).T))
    parts = [np.stack(first), middle, back, np.stack(last)]
    left = np.concatenate([np.cos(twist), np.sin(twist)], 1).astype(np.float32)
    for _ in range(3):
        parts.append(left.astype(jnp.bfloat16))
        left = left - parts[-1].astype(np.float32)
    return np.concatenate([a.reshape(-1, a.shape[-1]) for a in parts], 0)


def split(value):
    high = value.astype(jnp.bfloat16)
    return high, (value - high.astype(jnp.float32)).astype(jnp.bfloat16)


def dot(a, b):
    return jnp.dot(a, b, preferred_element_type=jnp.float32)


def pack_kernel(jobs, total, part, echoes, *refs):
    turn, outs, spread = lax.axis_index("turn"), refs[:-1], refs[-1]
    for k, (flip, row0, rows) in enumerate(jobs):
        for row in range(0, rows, 8):
            start = pl.multiple_of((turn ^ flip) * total + row0 + row, 8)
            for p in range(2):
                block = echoes[p, pl.ds(start, 8), :].astype(jnp.float32)
                for q in range(part):
                    spread[k, row // 8, p, q * 8 : (q + 1) * 8] = block[:, q * LANES : (q + 1) * LANES]
    for k, (flip, row0, rows) in enumerate(jobs):
        for row in range(rows):
            for p in range(2):
                for e in range(2):
                    start = e * 8 + row % 8
                    picked = spread[k, row // 8, p, pl.ds(start, part // 2, stride=16), :]
                    outs[k][p, row, e] = picked.astype(jnp.bfloat16)


def pack(echoes, jobs, total, cost):
    part = echoes.shape[2] // LANES
    vm = pl.BlockSpec(memory_space=pltpu.VMEM)
    tiles = max(rows for _, _, rows in jobs) // 8
    return pl.pallas_call(
        functools.partial(pack_kernel, tuple(jobs), total, part),
        in_specs=[vm],
        out_specs=[vm] * len(jobs),
        out_shape=[jax.ShapeDtypeStruct((2, rows, 2, part // 2, LANES), jnp.bfloat16) for _, _, rows in jobs],
        scratch_shapes=[pltpu.VMEM((len(jobs), tiles, 2, part * 8, LANES), jnp.float32)],
        compiler_params=pltpu.CompilerParams(vmem_limit_bytes=12 * 1024 * 1024),
        cost_estimate=pl.CostEstimate(flops=10**6, bytes_accessed=cost, transcendentals=0),
    )(echoes)


def order_kernel(width, strips, slow, dots, out, twist):
    me = lax.axis_index("turn") * strips + lax.axis_index("strip")
    size = dots.shape[1]
    row_ids = lax.broadcasted_iota(jnp.int32, (size, size), 0)
    col_ids = lax.broadcasted_iota(jnp.int32, (size, size), 1)
    order = jnp.where(row_ids == (col_ids ^ (me * width)), 1.0, 0.0).astype(jnp.bfloat16)
    out[...] = dot(dots[: 4 * size], order).astype(jnp.bfloat16)
    base = dots.shape[0] - 3 * slow
    terms = [dots[base + k * slow : base + (k + 1) * slow].astype(jnp.float32) for k in range(3)]
    twist[...] = terms[0] + terms[1] + terms[2]


def order_tables(dots, width, strips, slow):
    vm = pl.BlockSpec(memory_space=pltpu.VMEM)
    size = dots.shape[1]
    return pl.pallas_call(
        functools.partial(order_kernel, width, strips, slow),
        in_specs=[vm],
        out_specs=[vm, vm],
        out_shape=[
            jax.ShapeDtypeStruct((4 * size, size), jnp.bfloat16),
            jax.ShapeDtypeStruct((slow, 2 * LANES), jnp.float32),
        ],
        compiler_params=pltpu.CompilerParams(vmem_limit_bytes=8 * 1024 * 1024),
        cost_estimate=pl.CostEstimate(flops=10**6, bytes_accessed=2 * 10**6, transcendentals=0),
    )(dots)


def phase_kernel(total, slow, numbers, slow_cos, slow_sin, twist, out, slow_ramp, ids, sem):
    fetch = pltpu.make_async_copy(numbers, ids, sem)
    fetch.start()
    slow_ramp[0] = slow_cos[...].T
    slow_ramp[1] = slow_sin[...].T
    fetch.wait()
    for r in range(total):
        back = lax.rem(LANES - ids[total + r], LANES)
        for c in range(0, slow, 64):
            rows_c = slice(c, c + 64)
            tw_re = pltpu.roll(twist[rows_c, :LANES], back, 1)
            tw_im = pltpu.roll(twist[rows_c, LANES:], back, 1)
            u_re, u_im = slow_ramp[0, rows_c, r : r + 1], slow_ramp[1, rows_c, r : r + 1]
            out[r, rows_c, :LANES] = tw_re * u_re - tw_im * u_im
            out[r, rows_c, LANES:] = tw_re * u_im + tw_im * u_re


def phases(numbers, slow_cos, slow_sin, twist, total, slow):
    vm = pl.BlockSpec(memory_space=pltpu.VMEM)
    return pl.pallas_call(
        functools.partial(phase_kernel, total, slow),
        in_specs=[vm] * 4,
        out_specs=vm,
        out_shape=jax.ShapeDtypeStruct((total, slow, 2 * LANES), jnp.float32),
        scratch_shapes=[
            pltpu.VMEM((2, slow, total), jnp.float32),
            pltpu.SMEM(numbers.shape, jnp.int32),
            pltpu.SemaphoreType.DMA,
        ],
        compiler_params=pltpu.CompilerParams(vmem_limit_bytes=4 * 1024 * 1024),
        cost_estimate=pl.CostEstimate(flops=10**6, bytes_accessed=2 * 10**6, transcendentals=0),
    )(numbers, slow_cos, slow_sin, twist)


def turn_kernel(filters, out, turned):
    core = lax.axis_index("turn") % 2
    slabs = filters.shape[1]
    for p in range(2):
        for d in range(LANES):
            at = pl.multiple_of((2 * d + core) * LANES, LANES)
            lanes = filters[p, :, pl.ds(at, LANES)].astype(jnp.float32)
            for slab in range(slabs):
                turned[slab, p, d : d + 1, :] = lanes[slab : slab + 1]
    for p in range(2):
        for slab in range(slabs):
            out[slab, p] = turned[slab, p].T.astype(jnp.bfloat16)


def turn_filters(filters):
    vm = pl.BlockSpec(memory_space=pltpu.VMEM)
    shape = (filters.shape[1], 2, LANES, LANES)
    return pl.pallas_call(
        turn_kernel,
        in_specs=[vm],
        out_specs=vm,
        out_shape=jax.ShapeDtypeStruct(shape, jnp.bfloat16),
        scratch_shapes=[pltpu.VMEM(shape, jnp.float32)],
        compiler_params=pltpu.CompilerParams(vmem_limit_bytes=4 * 1024 * 1024),
        cost_estimate=pl.CostEstimate(flops=10**6, bytes_accessed=2 * 10**6, transcendentals=0),
    )(filters)


def focus_kernel(bases, pieces, earlier, rows, row0, slow, out_slow, *refs):
    sources = len(bases)
    slabs, blocks = refs[0], refs[1 : 1 + sources]
    own = refs[1 + sources : 1 + sources + pieces]
    other = refs[1 + sources + pieces : 1 + sources + 2 * pieces]
    phase, first_dots_ref, dots, twist = refs[1 + sources + 2 * pieces :][:4]
    rest = refs[5 + sources + 2 * pieces :]
    images, out = rest[:earlier], rest[earlier]
    s1, y1, s2, y2, s3, y3, s4, filt, ids, slab_sem = rest[earlier + 1 :][:10]
    fetch = pltpu.make_async_copy(slabs, ids, slab_sem)
    fetch.start()
    tile = out
    writes = []
    if earlier:
        tile, write_sem = rest[earlier + 11 :]
        for k, source in enumerate((*images, tile)):
            for p in range(2):
                writes.append(pltpu.make_async_copy(source.at[p], out.at[p, k], write_sem.at[2 * k + p]))
        for write in writes[:-2]:
            write.start()
    core = lax.axis_index("turn") % 2
    per_zone = own[0].shape[0]
    for k in range(pieces):
        filt[core, k * per_zone : (k + 1) * per_zone] = own[k][...]
        filt[1 - core, k * per_zone : (k + 1) * per_zone] = other[k][...]
    half = slow // 2
    wide = 2 * LANES
    first = [[first_dots_ref.at[pl.ds((2 * e + k) * slow, slow)] for k in range(2)] for e in range(2)]
    base = 4 * slow
    middle = [dots.at[pl.ds(base + k * wide, wide)] for k in range(2)]
    back = [dots.at[pl.ds(base + (2 + k) * wide, wide)] for k in range(2)]
    base += 4 * wide
    last = [[dots.at[pl.ds(base + (2 * e + k) * out_slow, out_slow)] for k in range(2)] for e in range(2)]

    def first_dots(pair):
        for e in range(2):
            data = jnp.concatenate(
                [
                    jnp.concatenate([block[p, base + r, e] for block, base in zip(blocks, bases) for p in range(2)], 0)
                    for r in (2 * pair, 2 * pair + 1)
                ],
                1,
            )
            s1[pair, e] = dot(first[e][0][...], data) + dot(first[e][1][...], data)

    def first_twist(pair):
        for i in range(2):
            lanes = slice(i * LANES, (i + 1) * LANES)
            for part in range(2):
                rows_c = slice(part * half, (part + 1) * half)
                even_re, even_im = s1[pair, 0, :half, lanes], s1[pair, 0, half:, lanes]
                odd_re, odd_im = s1[pair, 1, :half, lanes], s1[pair, 1, half:, lanes]
                if part == 0:
                    re, im = even_re + odd_re, even_im + odd_im
                else:
                    re, im = even_re - odd_re, even_im - odd_im
                tw_re, tw_im = twist[rows_c, :LANES], twist[rows_c, LANES:]
                (rh, rl), (ih, il) = split(re * tw_re + im * tw_im), split(im * tw_re - re * tw_im)
                y1[pair, i, rows_c] = jnp.concatenate([rh, ih, rl, il], 1)

    def lane_dots(pair, source, table, target):
        mix = source[pair].reshape(2 * slow, 2 * wide)
        target[pair] = (
            dot(mix[:, :wide], table[0][...]) + dot(mix[:, wide:], table[0][...]) + dot(mix[:, :wide], table[1][...])
        )

    def respond(pair):
        for i in range(2):
            r = row0 + 2 * pair + i
            slab = ids[r]
            for part in range(2):
                rows_s = slice(i * slow + part * half, i * slow + (part + 1) * half)
                re, im = s2[pair, rows_s, :LANES], s2[pair, rows_s, LANES:]
                h_re = filt[part, slab, 0].astype(jnp.float32)
                h_im = filt[part, slab, 1].astype(jnp.float32)
                re, im = re * h_re - im * h_im, re * h_im + im * h_re
                (rh, rl), (ih, il) = split(re), split(im)
                y2[pair, i, part * half : (part + 1) * half] = jnp.concatenate([rh, ih, rl, il], 1)

    def back_twist(pair):
        for i in range(2):
            r = row0 + 2 * pair + i
            lanes = slice(i * LANES, (i + 1) * LANES)
            parts = []
            for part in range(2):
                rows_c = slice(part * half, (part + 1) * half)
                rows_s = slice(i * slow + part * half, i * slow + (part + 1) * half)
                re, im = s3[pair, rows_s, :LANES], s3[pair, rows_s, LANES:]
                tw_re, tw_im = phase[r, rows_c, :LANES], phase[r, rows_c, LANES:]
                parts.append((re * tw_re - im * tw_im, re * tw_im + im * tw_re))
            (a_re, a_im), (b_re, b_im) = parts
            for e, (re, im) in enumerate(((a_re + b_re, a_im + b_im), (a_re - b_re, a_im - b_im))):
                (rh, rl), (ih, il) = split(re), split(im)
                y3[pair, e, 0, :, lanes] = jnp.concatenate([rh, ih], 0)
                y3[pair, e, 1, :, lanes] = jnp.concatenate([rl, il], 0)

    def last_dots(pair):
        for e in range(2):
            high, low = y3[pair, e, 0], y3[pair, e, 1]
            s4[pair, e] = (
                dot(last[e][0][...], high) + dot(last[e][1][...], high) + dot(last[e][0][...], low)
            )

    def store(pair):
        count = out_slow // 2
        for i in range(2):
            r = (row0 + 2 * pair + i) % 8
            turned = ids[ids.shape[0] // 2 + row0 + 2 * pair + i]
            for e in range(2):
                lanes = pltpu.roll(s4[pair, e, :, i * LANES : (i + 1) * LANES], turned, 1)
                for p in range(2):
                    for q in range(0, count, 8):
                        tile[p, pl.ds((2 * q + e) * 8 + r, 8, stride=16), :] = lanes[p * count + q : p * count + q + 8]

    steps = [
        first_dots,
        first_twist,
        lambda pair: lane_dots(pair, y1, middle, s2),
        respond,
        lambda pair: lane_dots(pair, y2, back, s3),
        back_twist,
        last_dots,
        store,
    ]
    streams = [[(step, pair) for pair in range(k, rows // 2, 2) for step in range(8)] for k in range(2)]
    fetch.wait()
    for t in range(len(streams[0]) + 1):
        now = [s[t - k] for k, s in enumerate(streams) if 0 <= t - k < len(s)]
        for step, pair in sorted(now, key=lambda job: job[0] % 2):
            steps[step](pair)
    for write in writes[-2:]:
        write.start()
    for write in writes:
        write.wait()


def focus(blocks, bases, own, other, tables, slabs, images, rows, row0, total, slow, out_slow, final):
    slots, pieces = rows // 2, len(own)

    def full(a):
        return pl.BlockSpec(a.shape, lambda i: (0,) * a.ndim)

    image = (2, out_slow * 8, LANES)
    shape = (2, total // 8, *image[1:]) if final else image
    operands = [slabs, *blocks, *own, *other, *tables, *images]
    extra = [pltpu.VMEM(image, jnp.float32), pltpu.SemaphoreType.DMA((total // 4,))] if final else []
    return pl.pallas_call(
        functools.partial(focus_kernel, tuple(bases), pieces, len(images), rows, row0, slow, out_slow),
        grid=(1,),
        in_specs=[full(a) for a in operands],
        out_specs=pl.BlockSpec(memory_space=pl.ANY) if final else pl.BlockSpec(image, lambda i: (0, 0, 0)),
        out_shape=jax.ShapeDtypeStruct(shape, jnp.float32),
        scratch_shapes=[
            pltpu.VMEM((slots, 2, slow, 2 * LANES), jnp.float32),
            pltpu.VMEM((slots, 2, slow, 4 * LANES), jnp.bfloat16),
            pltpu.VMEM((slots, 2 * slow, 2 * LANES), jnp.float32),
            pltpu.VMEM((slots, 2, slow, 4 * LANES), jnp.bfloat16),
            pltpu.VMEM((slots, 2 * slow, 2 * LANES), jnp.float32),
            pltpu.VMEM((slots, 2, 2, slow, 2 * LANES), jnp.bfloat16),
            pltpu.VMEM((slots, 2, out_slow, 2 * LANES), jnp.float32),
            pltpu.VMEM((2, pieces * own[0].shape[0], *own[0].shape[1:]), jnp.bfloat16),
            pltpu.SMEM(slabs.shape, jnp.int32),
            pltpu.SemaphoreType.DMA,
            *extra,
        ],
        compiler_params=pltpu.CompilerParams(vmem_limit_bytes=28 * 1024 * 1024),
        cost_estimate=pl.CostEstimate(flops=3 * 10**9, bytes_accessed=8 * 10**6, transcendentals=0),
    )(*operands)


def swap(value, axis, flip):
    size = lax.axis_size(axis)
    return lax.ppermute(value, axis, [(a, a ^ flip) for a in range(size)])


def per_device(echoes, filters, slab_index, shifts):
    turns, strips, zones = lax.axis_size("turn"), lax.axis_size("strip"), lax.axis_size("blk")
    strip, zone = lax.axis_index("strip"), lax.axis_index("blk")
    sources = turns * strips
    length = echoes.shape[2] * sources
    slow = length // LANES
    total = slab_index.shape[0]
    out_slow = slow // strips
    per_zone = filters.shape[1]
    width = slow // sources
    behind = (strips - strip) * (length // strips)
    echoes, zone, behind = lax.optimization_barrier((echoes, zone, behind))
    dots = jnp.asarray(tables(length, sources, length // strips))

    jobs = [[(0, 0, total)], [(1, 0, total)], []]
    starts = [sum(CHUNKS[:k]) for k in range(len(CHUNKS))]
    for k, rows in enumerate(CHUNKS):
        jobs[min(k + 1, 2)] += [(flip, starts[k], rows) for flip in range(2, turns)]
    sent = []
    for k, cost in enumerate((4 * 10**6, 4 * 10**6, 2 * 10**6)):
        sent += pack(echoes, jobs[k], total, cost)
    half = turn_filters(filters)
    first, twist = order_tables(dots, width, strips, slow)
    held = {}
    for (flip, start, rows), block in zip(sum(jobs, []), sent):
        if flip:
            block = swap(block, "turn", flip)
        for ds in range(strips):
            mine = swap(block, "strip", ds) if ds else block
            held[flip * strips + ds, start] = mine

    own = [half] + [swap(half, "blk", d) for d in range(1, zones)]
    other = [swap(piece, "turn", 1) for piece in own]
    local_slab = (slab_index // per_zone ^ zone) * per_zone + slab_index % per_zone

    c = jnp.arange(slow, dtype=jnp.int32)[None, :]
    offset = (shifts + behind) & (length - 1)
    c_angle = (offset[:, None] * c & (length - 1)).astype(jnp.float32) * (2.0 * math.pi / length)
    slow_ramp = (jnp.cos(c_angle), -jnp.sin(c_angle))
    numbers = jnp.concatenate([local_slab, shifts & (LANES - 1)])
    phase = phases(numbers, *slow_ramp, twist, total, slow)

    images = []
    for k, (start, rows) in enumerate(zip(starts, CHUNKS)):
        blocks, bases = [], []
        for slot in range(sources):
            whole = slot // strips < 2
            blocks.append(held[slot, 0 if whole else start])
            bases.append(start if whole else 0)
        final = k == len(CHUNKS) - 1
        image = focus(
            blocks, bases, own, other, (phase, first, dots, twist), numbers, images, rows, start, total, slow, out_slow, final
        )
        images.append(image)
    image = image.reshape(2, total // 8, out_slow, 8, LANES).transpose(0, 1, 3, 2, 4)
    return image.reshape(2, total, out_slow * LANES)


def solution(mesh):
    in_specs = (
        P(None, "blk", ("turn", "strip")),
        P(None, "blk", None),
        P(("blk", "turn")),
        P(("blk", "turn")),
    )
    out_specs = P(None, ("blk", "turn"), "strip")

    return jax.shard_map(per_device, mesh=mesh, in_specs=in_specs, out_specs=out_specs, check_vma=False)
```

```python
import functools
import math

import jax
import jax.numpy as jnp
import numpy as np
from jax import lax
from jax.experimental import pallas as pl
from jax.experimental.pallas import tpu as pltpu
from jax.sharding import PartitionSpec as P


LANES = 128
CHUNKS = (8, 8)


def hi_lo(table):
    high = table.astype(jnp.bfloat16)
    low = (table - high.astype(np.float64)).astype(jnp.bfloat16)
    return high, low


def block_matrix(phase, sign):
    cos, sin = np.cos(phase), sign * np.sin(phase)
    return np.concatenate([np.concatenate([cos, -sin], 1), np.concatenate([sin, cos], 1)], 0)


@functools.lru_cache(maxsize=None)
def tables(length, sources, out_len):
    slow = length // LANES
    half = slow // 2
    part = half // sources
    out_half = out_len // LANES // 2
    q = np.arange(slow)
    c = np.arange(half)
    lane = np.arange(LANES)
    lane_phase = 2 * np.pi * (lane[:, None] * lane[None, :] % LANES) / LANES
    twist = 2 * np.pi * (q[:, None] * lane[None, :]) / length
    first, last = [], []
    for parity in range(2):
        index = 2 * c + parity
        table = block_matrix(2 * np.pi * (c[:, None] * index[None, :] % slow) / slow, -1.0)
        table = table.reshape(slow, 2, sources, part).transpose(0, 2, 1, 3).reshape(slow, slow)
        first.append(np.stack(hi_lo(table)))
        table = block_matrix(2 * np.pi * (index[:out_half, None] * c[None, :] % slow) / slow, 1.0) / length
        last.append(np.stack(hi_lo(table)))
    middle = np.stack(hi_lo(block_matrix(lane_phase, -1.0).T))
    back = np.stack(hi_lo(block_matrix(lane_phase, 1.0).T))
    parts = [np.stack(first), middle, back, np.stack(last)]
    left = np.concatenate([np.cos(twist), np.sin(twist)], 1).astype(np.float32)
    for _ in range(3):
        parts.append(left.astype(jnp.bfloat16))
        left = left - parts[-1].astype(np.float32)
    return np.concatenate([a.reshape(-1, a.shape[-1]) for a in parts], 0)


def split(value):
    high = value.astype(jnp.bfloat16)
    return high, (value - high.astype(jnp.float32)).astype(jnp.bfloat16)


def dot(a, b):
    return jnp.dot(a, b, preferred_element_type=jnp.float32)


def pack_kernel(jobs, total, part, echoes, *refs):
    turn, outs, spread = lax.axis_index("turn"), refs[:-1], refs[-1]
    for k, (flip, row0, rows) in enumerate(jobs):
        for row in range(0, rows, 8):
            start = pl.multiple_of((turn ^ flip) * total + row0 + row, 8)
            for p in range(2):
                block = echoes[p, pl.ds(start, 8), :].astype(jnp.float32)
                for q in range(part):
                    spread[k, row // 8, p, q * 8 : (q + 1) * 8] = block[:, q * LANES : (q + 1) * LANES]
    for k, (flip, row0, rows) in enumerate(jobs):
        for row in range(rows):
            for p in range(2):
                for e in range(2):
                    start = e * 8 + row % 8
                    picked = spread[k, row // 8, p, pl.ds(start, part // 2, stride=16), :]
                    outs[k][p, row, e] = picked.astype(jnp.bfloat16)


def pack(echoes, jobs, total, cost):
    part = echoes.shape[2] // LANES
    vm = pl.BlockSpec(memory_space=pltpu.VMEM)
    tiles = max(rows for _, _, rows in jobs) // 8
    return pl.pallas_call(
        functools.partial(pack_kernel, tuple(jobs), total, part),
        in_specs=[vm],
        out_specs=[vm] * len(jobs),
        out_shape=[jax.ShapeDtypeStruct((2, rows, 2, part // 2, LANES), jnp.bfloat16) for _, _, rows in jobs],
        scratch_shapes=[pltpu.VMEM((len(jobs), tiles, 2, part * 8, LANES), jnp.float32)],
        compiler_params=pltpu.CompilerParams(vmem_limit_bytes=12 * 1024 * 1024),
        cost_estimate=pl.CostEstimate(flops=10**6, bytes_accessed=cost, transcendentals=0),
    )(echoes)


def order_kernel(width, strips, slow, dots, out, twist):
    me = lax.axis_index("turn") * strips + lax.axis_index("strip")
    size = dots.shape[1]
    row_ids = lax.broadcasted_iota(jnp.int32, (size, size), 0)
    col_ids = lax.broadcasted_iota(jnp.int32, (size, size), 1)
    order = jnp.where(row_ids == (col_ids ^ (me * width)), 1.0, 0.0).astype(jnp.bfloat16)
    out[...] = dot(dots[: 4 * size], order).astype(jnp.bfloat16)
    base = dots.shape[0] - 3 * slow
    terms = [dots[base + k * slow : base + (k + 1) * slow].astype(jnp.float32) for k in range(3)]
    twist[...] = terms[0] + terms[1] + terms[2]


def order_tables(dots, width, strips, slow):
    vm = pl.BlockSpec(memory_space=pltpu.VMEM)
    size = dots.shape[1]
    return pl.pallas_call(
        functools.partial(order_kernel, width, strips, slow),
        in_specs=[vm],
        out_specs=[vm, vm],
        out_shape=[
            jax.ShapeDtypeStruct((4 * size, size), jnp.bfloat16),
            jax.ShapeDtypeStruct((slow, 2 * LANES), jnp.float32),
        ],
        compiler_params=pltpu.CompilerParams(vmem_limit_bytes=8 * 1024 * 1024),
        cost_estimate=pl.CostEstimate(flops=10**6, bytes_accessed=2 * 10**6, transcendentals=0),
    )(dots)


def phase_kernel(total, slow, numbers, slow_cos, slow_sin, twist, out, slow_ramp, ids, sem):
    fetch = pltpu.make_async_copy(numbers, ids, sem)
    fetch.start()
    slow_ramp[0] = slow_cos[...].T
    slow_ramp[1] = slow_sin[...].T
    fetch.wait()
    for r in range(total):
        back = lax.rem(LANES - ids[total + r], LANES)
        for c in range(0, slow, 64):
            rows_c = slice(c, c + 64)
            tw_re = pltpu.roll(twist[rows_c, :LANES], back, 1)
            tw_im = pltpu.roll(twist[rows_c, LANES:], back, 1)
            u_re, u_im = slow_ramp[0, rows_c, r : r + 1], slow_ramp[1, rows_c, r : r + 1]
            out[r, rows_c, :LANES] = tw_re * u_re - tw_im * u_im
            out[r, rows_c, LANES:] = tw_re * u_im + tw_im * u_re


def phases(numbers, slow_cos, slow_sin, twist, total, slow):
    vm = pl.BlockSpec(memory_space=pltpu.VMEM)
    return pl.pallas_call(
        functools.partial(phase_kernel, total, slow),
        in_specs=[vm] * 4,
        out_specs=vm,
        out_shape=jax.ShapeDtypeStruct((total, slow, 2 * LANES), jnp.float32),
        scratch_shapes=[
            pltpu.VMEM((2, slow, total), jnp.float32),
            pltpu.SMEM(numbers.shape, jnp.int32),
            pltpu.SemaphoreType.DMA,
        ],
        compiler_params=pltpu.CompilerParams(vmem_limit_bytes=4 * 1024 * 1024),
        cost_estimate=pl.CostEstimate(flops=10**6, bytes_accessed=2 * 10**6, transcendentals=0),
    )(numbers, slow_cos, slow_sin, twist)


def turn_kernel(filters, out, turned):
    core = lax.axis_index("turn") % 2
    slabs = filters.shape[1]
    for p in range(2):
        for d in range(LANES):
            at = pl.multiple_of((2 * d + core) * LANES, LANES)
            lanes = filters[p, :, pl.ds(at, LANES)].astype(jnp.float32)
            for slab in range(slabs):
                turned[slab, p, d : d + 1, :] = lanes[slab : slab + 1]
    for p in range(2):
        for slab in range(slabs):
            out[slab, p] = turned[slab, p].T.astype(jnp.bfloat16)


def turn_filters(filters):
    vm = pl.BlockSpec(memory_space=pltpu.VMEM)
    shape = (filters.shape[1], 2, LANES, LANES)
    return pl.pallas_call(
        turn_kernel,
        in_specs=[vm],
        out_specs=vm,
        out_shape=jax.ShapeDtypeStruct(shape, jnp.bfloat16),
        scratch_shapes=[pltpu.VMEM(shape, jnp.float32)],
        compiler_params=pltpu.CompilerParams(vmem_limit_bytes=4 * 1024 * 1024),
        cost_estimate=pl.CostEstimate(flops=10**6, bytes_accessed=2 * 10**6, transcendentals=0),
    )(filters)


def focus_kernel(bases, pieces, earlier, rows, row0, slow, out_slow, *refs):
    sources = len(bases)
    slabs, blocks = refs[0], refs[1 : 1 + sources]
    count = 1 if earlier else 2 * pieces
    filters, rest = refs[1 + sources : 1 + sources + count], refs[1 + sources + count :]
    phase, first_dots_ref, dots, twist = rest[:4]
    images, out, rest = rest[4 : 4 + earlier], rest[4 + earlier], rest[5 + earlier :]
    filt, rest = (filters[0], rest) if earlier else (rest[0], rest[1:])
    s1, y1, s2, y2, s3, y3, s4, ids, slab_sem = rest[:9]
    fetch = pltpu.make_async_copy(slabs, ids, slab_sem)
    fetch.start()
    tile = out
    writes = []
    if earlier:
        tile, write_sem = rest[9:]
        for k, source in enumerate((*images, tile)):
            for p in range(2):
                writes.append(pltpu.make_async_copy(source.at[p], out.at[p, k], write_sem.at[2 * k + p]))
        for write in writes[:-2]:
            write.start()
    core = lax.axis_index("turn") % 2
    if not earlier:
        own, other = filters[:pieces], filters[pieces:]
        per_zone = own[0].shape[0]
        for k in range(pieces):
            filt[core, k * per_zone : (k + 1) * per_zone] = own[k][...]
            filt[1 - core, k * per_zone : (k + 1) * per_zone] = other[k][...]
    half = slow // 2
    wide = 2 * LANES
    first = [[first_dots_ref.at[pl.ds((2 * e + k) * slow, slow)] for k in range(2)] for e in range(2)]
    base = 4 * slow
    middle = [dots.at[pl.ds(base + k * wide, wide)] for k in range(2)]
    back = [dots.at[pl.ds(base + (2 + k) * wide, wide)] for k in range(2)]
    base += 4 * wide
    last = [[dots.at[pl.ds(base + (2 * e + k) * out_slow, out_slow)] for k in range(2)] for e in range(2)]

    def first_dots(pair):
        for e in range(2):
            data = jnp.concatenate(
                [
                    jnp.concatenate([block[p, base + r, e] for block, base in zip(blocks, bases) for p in range(2)], 0)
                    for r in (2 * pair, 2 * pair + 1)
                ],
                1,
            )
            both = dot(first_dots_ref[2 * e * slow : 2 * (e + 1) * slow], data)
            s1[pair, e] = both[:slow] + both[slow:]

    def first_twist(pair):
        for i in range(2):
            lanes = slice(i * LANES, (i + 1) * LANES)
            for part in range(2):
                rows_c = slice(part * half, (part + 1) * half)
                even_re, even_im = s1[pair, 0, :half, lanes], s1[pair, 0, half:, lanes]
                odd_re, odd_im = s1[pair, 1, :half, lanes], s1[pair, 1, half:, lanes]
                if part == 0:
                    re, im = even_re + odd_re, even_im + odd_im
                else:
                    re, im = even_re - odd_re, even_im - odd_im
                tw_re, tw_im = twist[rows_c, :LANES], twist[rows_c, LANES:]
                (rh, rl), (ih, il) = split(re * tw_re + im * tw_im), split(im * tw_re - re * tw_im)
                y1[pair, i, rows_c] = jnp.concatenate([rh, ih, rl, il], 1)

    def lane_dots(pair, source, table, target):
        mix = source[pair].reshape(2 * slow, 2 * wide)
        target[pair] = (
            dot(mix[:, :wide], table[0][...]) + dot(mix[:, wide:], table[0][...]) + dot(mix[:, :wide], table[1][...])
        )

    def respond(pair):
        for i in range(2):
            r = row0 + 2 * pair + i
            slab = ids[r]
            for part in range(2):
                rows_s = slice(i * slow + part * half, i * slow + (part + 1) * half)
                re, im = s2[pair, rows_s, :LANES], s2[pair, rows_s, LANES:]
                h_re = filt[part, slab, 0].astype(jnp.float32)
                h_im = filt[part, slab, 1].astype(jnp.float32)
                re, im = re * h_re - im * h_im, re * h_im + im * h_re
                (rh, rl), (ih, il) = split(re), split(im)
                y2[pair, i, part * half : (part + 1) * half] = jnp.concatenate([rh, ih, rl, il], 1)

    def back_twist(pair):
        for i in range(2):
            r = row0 + 2 * pair + i
            lanes = slice(i * LANES, (i + 1) * LANES)
            parts = []
            for part in range(2):
                rows_c = slice(part * half, (part + 1) * half)
                rows_s = slice(i * slow + part * half, i * slow + (part + 1) * half)
                re, im = s3[pair, rows_s, :LANES], s3[pair, rows_s, LANES:]
                tw_re, tw_im = phase[r, rows_c, :LANES], phase[r, rows_c, LANES:]
                parts.append((re * tw_re - im * tw_im, re * tw_im + im * tw_re))
            (a_re, a_im), (b_re, b_im) = parts
            for e, (re, im) in enumerate(((a_re + b_re, a_im + b_im), (a_re - b_re, a_im - b_im))):
                (rh, rl), (ih, il) = split(re), split(im)
                y3[pair, e, 0, :, lanes] = jnp.concatenate([rh, ih], 0)
                y3[pair, e, 1, :, lanes] = jnp.concatenate([rl, il], 0)

    def last_dots(pair):
        for e in range(2):
            high, low = y3[pair, e, 0], y3[pair, e, 1]
            both = dot(dots[base + 2 * e * out_slow : base + 2 * (e + 1) * out_slow], high)
            s4[pair, e] = both[:out_slow] + both[out_slow:] + dot(last[e][0][...], low)

    def store(pair):
        count = out_slow // 2
        for i in range(2):
            r = (row0 + 2 * pair + i) % 8
            turned = ids[ids.shape[0] // 2 + row0 + 2 * pair + i]
            for e in range(2):
                lanes = pltpu.roll(s4[pair, e, :, i * LANES : (i + 1) * LANES], turned, 1)
                for p in range(2):
                    for q in range(0, count, 8):
                        tile[p, pl.ds((2 * q + e) * 8 + r, 8, stride=16), :] = lanes[p * count + q : p * count + q + 8]

    steps = [
        first_dots,
        first_twist,
        lambda pair: lane_dots(pair, y1, middle, s2),
        respond,
        lambda pair: lane_dots(pair, y2, back, s3),
        back_twist,
        last_dots,
        store,
    ]
    count, late = 2, 1
    streams = [[(step, pair) for pair in range(k, rows // 2, count) for step in range(8)] for k in range(count)]
    fetch.wait()
    for t in range(len(streams[0]) + late * (count - 1)):
        now = [s[t - late * k] for k, s in enumerate(streams) if 0 <= t - late * k < len(s)]
        for step, pair in sorted(now, key=lambda job: job[0] % 2):
            steps[step](pair)
    for write in writes[-2:]:
        write.start()
    for write in writes:
        write.wait()


def focus(blocks, bases, filters, tables, slabs, images, rows, row0, total, slow, out_slow, final):
    slots, pieces = rows // 2, len(filters) // 2

    def full(a):
        return pl.BlockSpec(a.shape, lambda i: (0,) * len(a.shape))

    image = (2, out_slow * 8, LANES)
    shape = (2, total // 8, *image[1:]) if final else image
    operands = [slabs, *blocks, *filters, *tables, *images]
    out_shape = [jax.ShapeDtypeStruct(shape, jnp.float32)]
    out_specs = [pl.BlockSpec(memory_space=pl.ANY)]
    if not final:
        out_shape.append(jax.ShapeDtypeStruct((2, pieces * filters[0].shape[0], *filters[0].shape[1:]), jnp.bfloat16))
        out_specs = [full(a) for a in out_shape]
    extra = [pltpu.VMEM(image, jnp.float32), pltpu.SemaphoreType.DMA((total // 4,))] if final else []
    return pl.pallas_call(
        functools.partial(focus_kernel, tuple(bases), pieces, len(images), rows, row0, slow, out_slow),
        grid=(1,),
        in_specs=[full(a) for a in operands],
        out_specs=out_specs,
        out_shape=out_shape,
        scratch_shapes=[
            pltpu.VMEM((slots, 2, slow, 2 * LANES), jnp.float32),
            pltpu.VMEM((slots, 2, slow, 4 * LANES), jnp.bfloat16),
            pltpu.VMEM((slots, 2 * slow, 2 * LANES), jnp.float32),
            pltpu.VMEM((slots, 2, slow, 4 * LANES), jnp.bfloat16),
            pltpu.VMEM((slots, 2 * slow, 2 * LANES), jnp.float32),
            pltpu.VMEM((slots, 2, 2, slow, 2 * LANES), jnp.bfloat16),
            pltpu.VMEM((slots, 2, out_slow, 2 * LANES), jnp.float32),
            pltpu.SMEM(slabs.shape, jnp.int32),
            pltpu.SemaphoreType.DMA,
            *extra,
        ],
        compiler_params=pltpu.CompilerParams(vmem_limit_bytes=28 * 1024 * 1024),
        cost_estimate=pl.CostEstimate(flops=3 * 10**9, bytes_accessed=8 * 10**6, transcendentals=0),
    )(*operands)


def swap(value, axis, flip):
    size = lax.axis_size(axis)
    return lax.ppermute(value, axis, [(a, a ^ flip) for a in range(size)])


def per_device(echoes, filters, slab_index, shifts):
    turns, strips, zones = lax.axis_size("turn"), lax.axis_size("strip"), lax.axis_size("blk")
    strip, zone = lax.axis_index("strip"), lax.axis_index("blk")
    sources = turns * strips
    length = echoes.shape[2] * sources
    slow = length // LANES
    total = slab_index.shape[0]
    out_slow = slow // strips
    per_zone = filters.shape[1]
    width = slow // sources
    behind = (strips - strip) * (length // strips)
    echoes, zone, behind = lax.optimization_barrier((echoes, zone, behind))
    dots = jnp.asarray(tables(length, sources, length // strips))

    jobs = [[(0, 0, total)], [(1, 0, total)], []]
    starts = [sum(CHUNKS[:k]) for k in range(len(CHUNKS))]
    for k, rows in enumerate(CHUNKS):
        jobs[min(k + 1, 2)] += [(flip, starts[k], rows) for flip in range(2, turns)]
    sent = []
    for k, cost in enumerate((4 * 10**6, 4 * 10**6, 2 * 10**6)):
        sent += pack(echoes, jobs[k], total, cost)
    half = turn_filters(filters)
    first, twist = order_tables(dots, width, strips, slow)
    held = {}
    for (flip, start, rows), block in zip(sum(jobs, []), sent):
        if flip:
            block = swap(block, "turn", flip)
        for ds in range(strips):
            mine = swap(block, "strip", ds) if ds else block
            held[flip * strips + ds, start] = mine

    own = [half] + [swap(half, "blk", d) for d in range(1, zones)]
    other = [swap(piece, "turn", 1) for piece in own]
    local_slab = (slab_index // per_zone ^ zone) * per_zone + slab_index % per_zone

    c = jnp.arange(slow, dtype=jnp.int32)[None, :]
    offset = (shifts + behind) & (length - 1)
    c_angle = (offset[:, None] * c & (length - 1)).astype(jnp.float32) * (2.0 * math.pi / length)
    slow_ramp = (jnp.cos(c_angle), -jnp.sin(c_angle))
    numbers = jnp.concatenate([local_slab, shifts & (LANES - 1)])
    phase = phases(numbers, *slow_ramp, twist, total, slow)

    images, filt = [], [*own, *other]
    for k, (start, rows) in enumerate(zip(starts, CHUNKS)):
        blocks, bases = [], []
        for slot in range(sources):
            whole = slot // strips < 2
            blocks.append(held[slot, 0 if whole else start])
            bases.append(start if whole else 0)
        final = k == len(CHUNKS) - 1
        image, *given = focus(
            blocks, bases, filt, (phase, first, dots, twist), numbers, images, rows, start, total, slow, out_slow, final
        )
        images.append(image)
        filt = given
    image = image.reshape(2, total // 8, out_slow, 8, LANES).transpose(0, 1, 3, 2, 4)
    return image.reshape(2, total, out_slow * LANES)


def solution(mesh):
    in_specs = (
        P(None, "blk", ("turn", "strip")),
        P(None, "blk", None),
        P(("blk", "turn")),
        P(("blk", "turn")),
    )
    out_specs = P(None, ("blk", "turn"), "strip")

    return jax.shard_map(per_device, mesh=mesh, in_specs=in_specs, out_specs=out_specs, check_vma=False)
```
